256 devices in a mesh: grp: 4 (over y), chan: 64 (over x, z, core).
Axes of the slice: x: 4, y: 4, z: 8, core: 2. Of those that a mesh axis runs over, the one named last changes fastest.
Arguments:
- generator: bfloat16 [4, 64, 896, 896], P('grp', 'chan'), may hold values from -0.1875 to 0.1875
- hamiltonian: bfloat16 [4, 64, 896, 896], P('grp', 'chan'), may hold values from -6 to 6
- occupation: float32 [4, 64, 896], P('grp', 'chan'), may hold values from -1 to 1
- owner: int32 [4, 64, 49, 1], replicated, may hold values from 0 to 63; in each aligned block of 49 rows (0 to 48, 49 to 97, ..., all dimensions but the last counted through in order) at most 2 rows name the same one
- offset: int32 [4, 64, 49], replicated, may hold values from 0 to 48
Outputs:
- commutator: float32 [4, 64, 896, 896], P('grp', 'chan')
The draws below stay inside these ranges and needn't reach their ends.
Inputs may be any that keep to these rules, and one draw needn't show every extreme that they name: Among the 49 tiles of one channel, no owner is named more than 2 times; some owner exactly 2 times in some channels. Every owner receives a tile somewhere.
All inputs are finite; a program needn't handle non-finite values.
Results may differ from the reference program's by a relative error of at most 0.0042.
Values may be sent and summed in bfloat16 or wider, within the bound.
No kernel may reach another device: no remote copies, remote signals or barrier semaphores. Data moves between devices by JAX's collectives and lax.ppermute only.
A program may use at most 128 MiB of HBM per device.

```python
import math
import jax
import jax.numpy as jnp
import numpy as np

P_SIZE = 896
TILE = 128
NB = 7
NBLK = 49
MOST = 2
N_GRP = 4
N_CHAN = 64


def plant(entries, own_key, least, high):
    longest = entries.shape.index(max(entries.shape))
    spots = []
    for shift in (0, 1):
        where = [jax.random.randint(jax.random.fold_in(own_key, axis), (), 0, length) for axis, length in enumerate(entries.shape)]
        where[longest] = (where[longest] + shift) % entries.shape[longest]
        spots.append(tuple(where))
    return entries.at[spots[0]].set(least).at[spots[1]].set(high)


def level_of(rng, shape, pieces, smallest, top_value):
    def one(position, blocks):
        steps = jax.random.uniform(jax.random.fold_in(jax.random.fold_in(rng, 6), position), (blocks,), jnp.float32, smallest / len(pieces), top_value / len(pieces))
        return jnp.repeat(jnp.exp(steps), shape[position] // blocks).reshape((-1,) + (1,) * (len(shape) - position - 1))

    factor_of = one(*pieces[0])
    for cut in pieces[1:]:
        factor_of = factor_of * one(*cut)
    return factor_of


def routed_block(key, own, number, rows, amount, top, bound, skew):
    ranking = jax.random.permutation(key, amount)
    crowded, common = load_shares(amount, rows * top, bound, skew, True), load_shares(amount, rows * top, bound, skew, False)
    places = jnp.arange(amount)

    def named(sizes, rotation):
        used = int((sizes > 0).sum())
        fixed = max(1, used // 4)
        passed = fixed + (places - fixed + rotation * (used - fixed)) % max(1, amount - fixed)
        return jnp.zeros((amount,), jnp.int32).at[ranking[jnp.where(places < fixed, places, passed)]].set(jnp.asarray(sizes, jnp.int32))

    sizes = jnp.where(number % 4 == 0, named(crowded, number // 4), named(common, number - number // 4 - 1))
    mixed = jax.random.permutation(jax.random.fold_in(own, 3), amount)
    giver, receiver = mixed[0:amount // 2 * 2:2], mixed[1:amount // 2 * 2:2]
    room = jnp.minimum(sizes[giver] - 1, bound - sizes[receiver]) // 2
    room = jnp.where((giver == ranking[0]) | (receiver == ranking[0]) | (sizes[receiver] == 0), 0, jnp.maximum(room, 0))
    passed = jax.random.randint(jax.random.fold_in(own, 4), (amount // 2,), 0, 1 << 20) % (room + 1)
    sizes = sizes.at[giver].add(-passed).at[receiver].add(passed)
    items = jnp.searchsorted(jnp.cumsum(sizes), jnp.arange(rows * top), side="right").astype(jnp.int32)
    table = items.reshape(top, rows).T
    table = table[jax.random.permutation(jax.random.fold_in(own, 1), rows)]
    rotation = jax.random.randint(jax.random.fold_in(own, 2), (rows, 1), 0, top)
    return jnp.take_along_axis(table, (jnp.arange(top)[None, :] + rotation) % top, axis=1)


def load_shares(number_of, total, most, lean, full):
    loads = [(1 << 20) // math.isqrt(rank ** lean) + 1 for rank in range(1, number_of + 1)]
    largest = most if full else min(most, max(-(-total // number_of), total * loads[0] // sum(loads)))
    least = 1 if total - largest >= number_of - 1 else 0
    counts, surplus = [largest] + [least] * (number_of - 1), total - largest - least * (number_of - 1)
    while surplus > 0:
        candidates = [i for i in range(1, number_of) if counts[i] < largest] or [i for i in range(1, number_of) if counts[i] < most]
        mass, remaining = sum([loads[i] for i in candidates]), surplus
        for i in candidates:
            addition = min(most - counts[i], max(1, remaining * loads[i] // mass), surplus)
            counts[i] = counts[i] + addition
            surplus = surplus - addition
    return np.array(counts)


def gaussian(own_key, extent, deviation, bound, pieces=(), held_as=jnp.bfloat16):
    loudness = level_of(own_key, extent, pieces, -0.22, 0.18) if pieces else 1.0
    result = jax.random.normal(own_key, extent, jnp.float32) * deviation * loudness
    return jnp.minimum(jnp.maximum(result, -bound), bound).astype(held_as)


def setup_inputs(seed: int = 0) -> dict:
    key_of = jax.random.split(jax.random.key(seed), 6)
    generator = gaussian(key_of[0], (N_GRP, N_CHAN, P_SIZE, P_SIZE), (P_SIZE ** -0.5), 0.1875, ((0, 4), (1, 64)))
    hamiltonian = gaussian(key_of[1], (N_GRP, N_CHAN, P_SIZE, P_SIZE), 1.0, 6.0, ((0, 4), (1, 64)))
    occupation = jnp.clip(jax.random.uniform(key_of[2], (N_GRP, N_CHAN, P_SIZE), jnp.float32, -1.0, 1.0) * level_of(key_of[2], (N_GRP, N_CHAN, P_SIZE), ((0, 4), (1, 64)), -0.4, 0.0), -1.0, 1.0)
    owner_keys = jax.random.split(jax.random.fold_in(key_of[3], 1), N_GRP * N_CHAN * NBLK // NBLK)
    owner_turns = jax.random.permutation(jax.random.fold_in(key_of[3], 3), N_GRP * N_CHAN * NBLK // NBLK)
    owner = jax.vmap(lambda own, number: routed_block(jax.random.fold_in(key_of[3], 2), own, number, NBLK, N_CHAN, 1, MOST, 2))(owner_keys, owner_turns).reshape((N_GRP, N_CHAN, NBLK, 1))
    offset = plant(jax.random.randint(key_of[4], (N_GRP, N_CHAN, NBLK), 0, NBLK), jax.random.fold_in(key_of[4], 1), 0, NBLK - 1).astype(jnp.int32)
    return {"generator": generator, "hamiltonian": hamiltonian, "occupation": occupation, "owner": owner, "offset": offset}


def to_blocks(matrix):
    lead = matrix.shape[:-2]
    grid = matrix.reshape(lead + (NB, TILE, NB, TILE))
    grid = jnp.swapaxes(grid, -3, -2)
    return grid.reshape(lead + (NB * NB, TILE * TILE))


def from_blocks(blocks):
    lead = blocks.shape[:-2]
    grid = blocks.reshape(lead + (NB, NB, TILE, TILE))
    grid = jnp.swapaxes(grid, -3, -2)
    return grid.reshape(lead + (NB * TILE, NB * TILE))


def reference(generator, hamiltonian, occupation, owner, offset):
    ladders = []
    recoupled = []
    for group in range(N_GRP):
        gen_mat = generator[group]
        ham_mat = hamiltonian[group]
        occ_row = occupation[group]
        gen_occ = (gen_mat.astype(jnp.float32) * occ_row[:, None, :]).astype(jnp.bfloat16)
        ham_occ = (ham_mat.astype(jnp.float32) * occ_row[:, None, :]).astype(jnp.bfloat16)
        ladder = jnp.einsum("cij,cjk->cik", gen_occ.astype(jnp.float32), ham_mat.astype(jnp.float32))
        ladder = ladder - jnp.einsum("cij,cjk->cik", ham_occ.astype(jnp.float32), gen_mat.astype(jnp.float32))
        ladders.append(ladder)
        segment = (owner[group, :, :, 0] * NBLK + offset[group]).reshape(-1).astype(jnp.int32)
        gen_tiles = to_blocks(gen_mat).reshape(N_CHAN * NBLK, TILE * TILE).astype(jnp.float32)
        ham_tiles = to_blocks(ham_mat).reshape(N_CHAN * NBLK, TILE * TILE).astype(jnp.float32)
        gen_ph = jax.ops.segment_sum(gen_tiles, segment, num_segments=N_CHAN * NBLK).astype(jnp.bfloat16)
        ham_ph = jax.ops.segment_sum(ham_tiles, segment, num_segments=N_CHAN * NBLK).astype(jnp.bfloat16)
        gen_full = from_blocks(gen_ph.reshape(N_CHAN, NBLK, TILE * TILE)).astype(jnp.float32)
        ham_full = from_blocks(ham_ph.reshape(N_CHAN, NBLK, TILE * TILE)).astype(jnp.float32)
        cross = jnp.einsum("cij,cjk->cik", gen_full, ham_full) - jnp.einsum("cij,cjk->cik", ham_full, gen_full)
        cross_tiles = to_blocks(cross).reshape(N_CHAN * NBLK, TILE * TILE)
        picked = jnp.take(cross_tiles, segment, axis=0)
        recoupled.append(from_blocks(picked.reshape(N_CHAN, NBLK, TILE * TILE)))
    results = []
    for group in range(N_GRP):
        partner = recoupled[group ^ 1]
        results.append(ladders[group] + recoupled[group] - jnp.swapaxes(partner, -1, -2))
    return jnp.stack(results)
```

```python
import functools

import jax
import jax.numpy as jnp
from jax import lax
from jax.experimental import pallas as pl
from jax.experimental.pallas import tpu as pltpu
from jax.sharding import PartitionSpec as P

TILE = 128
SIDE = 7
BLOCKS = SIDE * SIDE
X, Z, CORE = 4, 8, 2
CHAN = X * Z * CORE
F32, BF16 = jnp.float32, jnp.bfloat16


SMEM = pl.BlockSpec(memory_space=pltpu.SMEM)
VMEM = pl.BlockSpec(memory_space=pltpu.VMEM)


def chan_of(x, z, core):
    return (x * Z + z) * CORE + core


def z_shift(value, step):
    pairs = [
        (chan_of(x, z, c), chan_of(x, (z + step) % Z, c))
        for x in range(X)
        for z in range(Z)
        for c in range(CORE)
    ]
    return lax.ppermute(value, "chan", pairs)


def x_shift(value, step, flip):
    pairs = [
        (chan_of(x, z, c), chan_of((x + step) % X, z, c ^ flip))
        for x in range(X)
        for z in range(Z)
        for c in range(CORE)
    ]
    return lax.ppermute(value, "chan", pairs)


def exchanged(value):
    return lax.all_to_all(value, "chan", split_axis=0, concat_axis=0, tiled=True)


def kernel_call(body, tables, arrays, outs, scratch=(), cost=(0, 0)):
    return pl.pallas_call(
        body,
        out_shape=outs,
        in_specs=[SMEM] * len(tables) + [VMEM] * len(arrays),
        out_specs=jax.tree.map(lambda _: VMEM, outs),
        scratch_shapes=list(scratch),
        cost_estimate=pl.CostEstimate(flops=cost[0], bytes_accessed=cost[1], transcendentals=0),
    )(*tables, *arrays)


def tile_at(ref, block):
    row = pl.multiple_of((block // SIDE) * TILE, TILE)
    col = pl.multiple_of((block % SIDE) * TILE, TILE)
    return ref[pl.ds(row, TILE), pl.ds(col, TILE)]


def send_tiles(main_blocks, second_blocks, gen, ham):
    count, extra = main_blocks.shape[0], second_blocks.shape[0]

    def body(main_table, second_table, gen_ref, ham_ref, main_ref, *second_refs):
        @pl.loop(0, count)
        def _(slot):
            block = main_table[slot]
            main_ref[slot, 0] = tile_at(gen_ref, block)
            main_ref[slot, 1] = tile_at(ham_ref, block)

        for step in range(extra):
            block = second_table[step]
            second_refs[step][0] = tile_at(gen_ref, block)
            second_refs[step][1] = tile_at(ham_ref, block)

    outs = [jax.ShapeDtypeStruct((count, 2, TILE, TILE), BF16)]
    outs += [jax.ShapeDtypeStruct((2, TILE, TILE), BF16)] * extra
    return kernel_call(body, (main_blocks, second_blocks), (gen, ham), outs)


def direct_tiles(blocks, gen, ham):
    def body(table, gen_ref, ham_ref, out_ref):
        @pl.loop(0, CHAN)
        def _(slot):
            block = table[slot]
            out_ref[slot, 0] = tile_at(gen_ref, block)
            out_ref[slot, 1] = tile_at(ham_ref, block)

    out = jax.ShapeDtypeStruct((CHAN, 2, TILE, TILE), BF16)
    return kernel_call(body, (blocks,), (gen, ham), out)


def placed(main_offsets, second_offsets, main, seconds):
    parts = len(seconds)
    each = seconds[0].shape[0]

    def body(main_table, second_table, main_ref, *refs):
        second_refs, (gen_ref, ham_ref, total) = refs[:parts], refs[parts:]
        total[...] = jnp.zeros_like(total)

        @pl.loop(0, CHAN)
        def _(slot):
            place = main_table[slot]

            @pl.when(place >= 0)
            def _():
                total[place] += main_ref[slot].astype(F32)

        for part in range(parts):

            @pl.loop(0, each)
            def _(slot):
                place = second_table[part * each + slot]

                @pl.when(place >= 0)
                def _():
                    total[place] += second_refs[part][slot].astype(F32)

        for i in range(SIDE):
            for j in range(SIDE):
                rows, cols = pl.ds(i * TILE, TILE), pl.ds(j * TILE, TILE)
                gen_ref[rows, cols] = total[i * SIDE + j, 0].astype(BF16)
                ham_ref[rows, cols] = total[i * SIDE + j, 1].astype(BF16)

    outs = [jax.ShapeDtypeStruct((SIDE * TILE, SIDE * TILE), BF16)] * 2
    scratch = [pltpu.VMEM((BLOCKS, 2, TILE, TILE), F32)]
    return kernel_call(body, (main_offsets, second_offsets), (main, *seconds), outs, scratch)


def back_tiles(main_offsets, second_offsets, cross, parts, each):
    def body(main_table, second_table, cross_ref, main_ref, *second_refs):
        @pl.loop(0, CHAN)
        def _(slot):
            main_ref[slot] = tile_at(cross_ref, main_table[slot]).astype(BF16)

        for part in range(parts):

            @pl.loop(0, each)
            def _(slot):
                block = second_table[part * each + slot]
                second_refs[part][slot] = tile_at(cross_ref, block).astype(BF16)

    outs = [jax.ShapeDtypeStruct((CHAN, TILE, TILE), BF16)]
    outs += [jax.ShapeDtypeStruct((each, TILE, TILE), BF16)] * parts
    return kernel_call(body, (main_offsets, second_offsets), (cross,), outs)


def back_direct(offsets, cross):
    def body(table, cross_ref, out_ref):
        @pl.loop(0, CHAN)
        def _(slot):
            out_ref[slot] = tile_at(cross_ref, table[slot]).astype(BF16)

    out = jax.ShapeDtypeStruct((CHAN, TILE, TILE), BF16)
    return kernel_call(body, (offsets,), (cross,), out)


def chosen(choice, arrays):
    count = len(arrays)

    def body(table, *refs):
        for step in range(Z):
            for part in range(count):

                @pl.when(table[step] == part)
                def _():
                    refs[count + step][...] = refs[part][step]

    outs = [jax.ShapeDtypeStruct((TILE, TILE), BF16)] * Z
    return kernel_call(body, (choice,), arrays, outs)


def gathered(slots, main, seconds):
    parts = len(seconds)
    each = 1 if seconds[0].ndim == 2 else seconds[0].shape[0]

    def body(table, main_ref, *refs):
        second_refs, out_ref, held = refs[:parts], refs[parts], refs[parts + 1]
        for part in range(parts):
            if each == 1:
                held[part] = second_refs[part][...]
            else:
                held[...] = second_refs[part][...]

        @pl.loop(0, BLOCKS)
        def _(block):
            slot = table[block]

            @pl.when(slot < CHAN)
            def _():
                out_ref[block] = main_ref[slot]

            @pl.when(slot >= CHAN)
            def _():
                out_ref[block] = held[slot - CHAN]

    out = jax.ShapeDtypeStruct((BLOCKS, TILE, TILE), BF16)
    scratch = [pltpu.VMEM((parts * each, TILE, TILE), BF16)]
    return kernel_call(body, (slots,), (main, *seconds), out, scratch)


def assembled(ladder, own, partner):
    own = own.reshape(SIDE, SIDE, TILE, TILE)
    partner = partner.reshape(SIDE, SIDE, TILE, TILE)

    def body(ladder_ref, own_ref, partner_ref, out_ref):
        for j in range(SIDE):
            cols = pl.ds(j * TILE, TILE)
            turned = partner_ref[j, 0].astype(F32).T
            out_ref[:, cols] = ladder_ref[:, cols] + own_ref[0, j].astype(F32) - turned

    side = SIDE * TILE
    return pl.pallas_call(
        body,
        grid=(SIDE,),
        out_shape=jax.ShapeDtypeStruct((side, side), F32),
        in_specs=[
            pl.BlockSpec((TILE, side), lambda i: (i, 0)),
            pl.BlockSpec((1, SIDE, TILE, TILE), lambda i: (i, 0, 0, 0)),
            pl.BlockSpec((SIDE, 1, TILE, TILE), lambda i: (0, i, 0, 0)),
        ],
        out_specs=pl.BlockSpec((TILE, side), lambda i: (i, 0)),
    )(ladder, own, partner)


def pair_product(left_a, right_a, left_b, right_b):
    first = jnp.dot(left_a, right_a, preferred_element_type=F32)
    return first - jnp.dot(left_b, right_b, preferred_element_type=F32)


def ladder_term(gen_mat, ham_mat, occ_row):
    gen_occ = (gen_mat.astype(F32) * occ_row[None, :]).astype(BF16)
    ham_occ = (ham_mat.astype(F32) * occ_row[None, :]).astype(BF16)
    return pair_product(gen_occ, ham_mat, ham_occ, gen_mat)


def homes_of(owner_map):
    names = jnp.arange(CHAN, dtype=jnp.int32)
    tiles = jnp.sum((owner_map[..., None] == names).astype(jnp.int32), axis=-2)
    double = tiles == 2
    load = jnp.sum(double.astype(jnp.int32), axis=-2)
    mine, other = load[..., :, None], load[..., None, :]
    ahead = (other > mine) | ((other == mine) & (names[None, :] < names[:, None]))
    rank = jnp.sum(ahead.astype(jnp.int32), axis=-1)
    return rank, double


def on_device(generator, hamiltonian, occupation, owner, offset):
    gen_mat, ham_mat, occ_row = generator[0, 0], hamiltonian[0, 0], occupation[0, 0]
    me, grp = lax.axis_index("chan"), lax.axis_index("grp")
    my_x, my_z, my_core = me // (Z * CORE), (me // CORE) % Z, me % CORE
    owner_all = owner[:, :, :, 0]
    owners = lax.dynamic_index_in_dim(owner_all, grp, 0, keepdims=False)
    offsets = lax.dynamic_index_in_dim(offset, grp, 0, keepdims=False)
    names = jnp.arange(CHAN, dtype=jnp.int32)
    blocks = jnp.arange(BLOCKS, dtype=jnp.int32)
    steps = jnp.arange(Z, dtype=jnp.int32)

    rank, _ = homes_of(owners)
    row, col = rank // Z, rank % Z
    home = chan_of(row // CORE, col, row % CORE)
    dest = jnp.sum(jnp.where(owners[:, :, None] == names, home, 0), axis=-1)
    alike = (owners[:, None, :] == owners[:, :, None]) & (blocks[None, :] < blocks[:, None])
    later = jnp.any(alike, axis=-1)
    plane = (dest // CORE) % Z

    rank_all, double_all = homes_of(owner_all)
    in_plane = double_all[..., None] & ((rank_all % Z)[:, None, :, None] == steps)
    crowded = jnp.max(jnp.sum(in_plane.astype(jnp.int32), axis=2)) > 1

    my_dest = lax.dynamic_index_in_dim(dest, me, 0, keepdims=False)
    my_later = lax.dynamic_index_in_dim(later, me, 0, keepdims=False)
    my_plane = (my_dest // CORE) % Z
    to_home = my_dest[None, :] == names[:, None]
    main_blocks = jnp.max(jnp.where(to_home & ~my_later, blocks, 0), axis=1)
    direct_blocks = jnp.max(jnp.where(to_home & my_later, blocks, 0), axis=1)
    to_plane = my_plane[None, :] == ((my_z + steps) % Z)[:, None]
    second_blocks = jnp.max(jnp.where(to_plane & my_later, blocks, 0), axis=1)

    main_send, *second_send = send_tiles(main_blocks, second_blocks, gen_mat, ham_mat)
    main = exchanged(main_send)
    ladder = ladder_term(gen_mat, ham_mat, occ_row)

    second_z = jnp.stack([second_send[0]] + [z_shift(second_send[s], s) for s in range(1, Z)])
    same = [second_z] + [x_shift(second_z, s, 0) for s in range(1, X)]
    seconds = same + [x_shift(part, 0, 1) for part in same]

    here = dest == me
    main_place = jnp.max(jnp.where(here & ~later, offsets, -1), axis=1)
    second_place = jnp.max(jnp.where(here & later, offsets, -1), axis=1)
    flips = jnp.arange(CORE, dtype=jnp.int32)[:, None, None]
    shifts = jnp.arange(X, dtype=jnp.int32)[None, :, None]
    from_z = ((my_z - steps) % Z)[None, None, :]
    came_from = chan_of((my_x - shifts) % X, from_z, my_core ^ flips).reshape(-1)
    goes_to = chan_of((my_x + shifts) % X, from_z, my_core ^ flips).reshape(-1)
    place_in = jnp.sum(jnp.where(came_from[:, None] == names, second_place, 0), axis=1)
    place_out = jnp.sum(jnp.where(goes_to[:, None] == names, second_place, 0), axis=1)

    def fast_place():
        return placed(main_place, place_in, main, seconds)

    def slow_place():
        arrived = exchanged(direct_tiles(direct_blocks, gen_mat, ham_mat))
        return placed(main_place, second_place, main, [arrived])

    gen_full, ham_full = lax.cond(crowded, slow_place, fast_place)
    cross = pair_product(gen_full, ham_full, ham_full, gen_full)

    back_main, *back_second = back_tiles(
        jnp.maximum(main_place, 0), jnp.maximum(place_out, 0), cross, X * CORE, Z
    )
    main_back = exchanged(back_main)
    routed = [back_second[0]]
    for flip in range(CORE):
        for step in range(X):
            if flip or step:
                routed.append(x_shift(back_second[flip * X + step], step, flip))
    line = chan_of(my_x, (my_z - steps) % Z, my_core)
    line_dest = jnp.where((line[:, None] == names)[:, :, None] & later[None], dest[None], -1)
    line_here = (line_dest >= 0) & ((line_dest // CORE) % Z == my_z)
    holder = jnp.max(jnp.where(line_here, line_dest, 0), axis=(1, 2))
    choice = ((holder % CORE) ^ my_core) * X + (my_x - holder // (Z * CORE)) % X
    picked = chosen(choice, routed)
    second_back = [picked[0]] + [z_shift(picked[s], Z - s) for s in range(1, Z)]

    fast_slots = jnp.where(my_later, CHAN + (my_plane - my_z) % Z, my_dest)
    slow_slots = jnp.where(my_later, CHAN + my_dest, my_dest)

    def fast_gather():
        return gathered(fast_slots, main_back, second_back)

    def slow_gather():
        arrived = exchanged(back_direct(jnp.maximum(second_place, 0), cross))
        return gathered(slow_slots, main_back, [arrived])

    own = lax.cond(crowded, slow_gather, fast_gather)
    mirror = [(g, g ^ 1) for g in range(lax.axis_size("grp"))]
    partner = lax.ppermute(own, "grp", mirror)
    return assembled(ladder, own, partner)[None, None]


def solution(mesh):
    in_specs = (
        P("grp", "chan", None, None),
        P("grp", "chan", None, None),
        P("grp", "chan", None),
        P(),
        P(),
    )
    out_specs = P("grp", "chan", None, None)
    return jax.shard_map(
        on_device, mesh=mesh, in_specs=in_specs, out_specs=out_specs, check_vma=False
    )
```

```python
import jax
import jax.numpy as jnp
from jax import lax
from jax.experimental import pallas as pl
from jax.experimental.pallas import tpu as pltpu
from jax.sharding import PartitionSpec as P


TILE = 128
SIDE = 7
BLOCKS = SIDE * SIDE
X, Z, CORE = 4, 8, 2
CHAN = X * Z * CORE
UPPER = 112
LIMIT = 24
PIECE = TILE // (X * CORE)
RELATIVE = [(step, flip) for flip in range(CORE) for step in range(X)]
F32, BF16 = jnp.float32, jnp.bfloat16


SMEM = pl.BlockSpec(memory_space=pltpu.SMEM)
VMEM = pl.BlockSpec(memory_space=pltpu.VMEM)


def chan_of(x, z, core):
    return (x * Z + z) * CORE + core


def z_shift(value, step):
    pairs = [
        (chan_of(x, z, c), chan_of(x, (z + step) % Z, c))
        for x in range(X)
        for z in range(Z)
        for c in range(CORE)
    ]
    return lax.ppermute(value, "chan", pairs)


def x_shift(value, step, flip):
    pairs = [
        (chan_of(x, z, c), chan_of((x + step) % X, z, c ^ flip))
        for x in range(X)
        for z in range(Z)
        for c in range(CORE)
    ]
    return lax.ppermute(value, "chan", pairs)


def exchanged(value):
    return lax.all_to_all(value, "chan", split_axis=0, concat_axis=0, tiled=True)


def kernel_call(body, tables, arrays, outs, scratch=(), cost=(0, 0)):
    return pl.pallas_call(
        body,
        out_shape=outs,
        in_specs=[SMEM] * len(tables) + [VMEM] * len(arrays),
        out_specs=jax.tree.map(lambda _: VMEM, outs),
        scratch_shapes=list(scratch),
        cost_estimate=pl.CostEstimate(flops=cost[0], bytes_accessed=cost[1], transcendentals=0),
        compiler_params=pltpu.CompilerParams(vmem_limit_bytes=LIMIT << 20),
    )(*tables, *arrays)


def tile_at(ref, block):
    row = pl.multiple_of((block // SIDE) * TILE, TILE)
    col = pl.multiple_of((block % SIDE) * TILE, TILE)
    return ref[pl.ds(row, TILE), pl.ds(col, TILE)]


def second_tiles(blocks, gen, ham):
    count = blocks.shape[0]

    def body(table, gen_ref, ham_ref, *refs):
        outs, arrived = refs[:count], refs[count]
        copies = []
        for step in range(count):
            block = table[step]
            row = pl.multiple_of((block // SIDE) * TILE, TILE)
            col = pl.multiple_of((block % SIDE) * TILE, TILE)
            for which, ref in enumerate((gen_ref, ham_ref)):
                source = ref.at[pl.ds(row, TILE), pl.ds(col, TILE)]
                copies.append(
                    pltpu.make_async_copy(source, outs[step].at[which], arrived.at[step, which])
                )
        for copy in copies:
            copy.start()
        for copy in copies:
            copy.wait()

    return pl.pallas_call(
        body,
        out_shape=[jax.ShapeDtypeStruct((2, TILE, TILE), BF16)] * count,
        in_specs=[SMEM, pl.BlockSpec(memory_space=pl.ANY), pl.BlockSpec(memory_space=pl.ANY)],
        out_specs=[VMEM] * count,
        scratch_shapes=[pltpu.SemaphoreType.DMA((count, 2))],
        compiler_params=pltpu.CompilerParams(vmem_limit_bytes=LIMIT << 20),
    )(blocks, gen, ham)


def direct_tiles(blocks, gen, ham):
    def body(table, gen_ref, ham_ref, out_ref):
        @pl.loop(0, CHAN)
        def _(slot):
            block = table[slot]
            out_ref[slot, 0] = tile_at(gen_ref, block)
            out_ref[slot, 1] = tile_at(ham_ref, block)

    out = jax.ShapeDtypeStruct((CHAN, 2, TILE, TILE), BF16)
    return kernel_call(body, (blocks,), (gen, ham), out)


def placed(main_offsets, second_offsets, main, seconds):
    parts = len(seconds)
    each = seconds[0].shape[0]

    def body(main_table, second_table, main_ref, *refs):
        second_refs, (gen_ref, ham_ref, total) = refs[:parts], refs[parts:]

        @pl.loop(0, BLOCKS)
        def _(block):
            total[block] = jnp.zeros((2, TILE, TILE), F32)

        @pl.loop(0, CHAN)
        def _(slot):
            place = main_table[slot]

            @pl.when(place >= 0)
            def _():
                total[place] += main_ref[slot].astype(F32)

        for part in range(parts):

            @pl.loop(0, each)
            def _(slot):
                place = second_table[part * each + slot]

                @pl.when(place >= 0)
                def _():
                    total[place] += second_refs[part][slot].astype(F32)

        @pl.loop(0, BLOCKS)
        def _(block):
            rows = pl.ds(pl.multiple_of((block // SIDE) * TILE, TILE), TILE)
            cols = pl.ds(pl.multiple_of((block % SIDE) * TILE, TILE), TILE)
            gen_ref[rows, cols] = total[block, 0].astype(BF16)
            ham_ref[rows, cols] = total[block, 1].astype(BF16)

    outs = [jax.ShapeDtypeStruct((SIDE * TILE, SIDE * TILE), BF16)] * 2
    scratch = [pltpu.VMEM((BLOCKS, 2, TILE, TILE), F32)]
    return kernel_call(body, (main_offsets, second_offsets), (main, *seconds), outs, scratch)


def back_tiles(main_offsets, second_offsets, pieces, cross):
    count = len(RELATIVE)

    def body(main_table, second_table, piece_table, cross_ref, upper_ref, lower_ref, *piece_refs):
        @pl.loop(0, CHAN)
        def _(slot):
            tile = tile_at(cross_ref, main_table[slot]).astype(BF16)
            upper_ref[slot] = tile[:UPPER]
            lower_ref[slot] = tile[UPPER:]
            block = second_table[slot]

            @pl.when(block >= 0)
            def _():
                row = (block // SIDE) * TILE
                col = pl.multiple_of((block % SIDE) * TILE, TILE)
                for part in range(count):
                    first = pl.multiple_of(row + piece_table[part] * PIECE, PIECE)
                    rows = cross_ref[pl.ds(first, PIECE), pl.ds(col, TILE)]
                    piece_refs[part][slot] = rows.astype(BF16)

    outs = [
        jax.ShapeDtypeStruct((CHAN, UPPER, TILE), BF16),
        jax.ShapeDtypeStruct((CHAN, TILE - UPPER, TILE), BF16),
    ]
    outs += [jax.ShapeDtypeStruct((CHAN, PIECE, TILE), BF16)] * count
    return kernel_call(body, (main_offsets, second_offsets, pieces), (cross,), outs)


def back_direct(offsets, cross):
    def body(table, cross_ref, out_ref):
        @pl.loop(0, CHAN)
        def _(slot):
            out_ref[slot] = tile_at(cross_ref, table[slot]).astype(BF16)

    out = jax.ShapeDtypeStruct((CHAN, TILE, TILE), BF16)
    return kernel_call(body, (offsets,), (cross,), out)


def joined(choice, lower, routed):
    rows = TILE - UPPER

    def body(table, lower_ref, *refs):
        routed_refs, out_ref = refs[:-1], refs[-1]

        @pl.loop(0, CHAN)
        def _(slot):
            out_ref[slot, :rows] = lower_ref[slot]
            part_of = table[slot]
            for part, ref in enumerate(routed_refs):

                @pl.when(part_of == part)
                def _():
                    out_ref[slot, rows:] = ref[slot]

    out = jax.ShapeDtypeStruct((CHAN, rows + PIECE, TILE), BF16)
    return kernel_call(body, (choice,), (lower, *routed), out)


def gathered(slots, main):
    def body(table, main_ref, out_ref):
        @pl.loop(0, BLOCKS)
        def _(block):
            slot = table[block]

            @pl.when(slot >= 0)
            def _():
                out_ref[block] = main_ref[slot]

    out = jax.ShapeDtypeStruct((BLOCKS, *main.shape[1:]), BF16)
    return kernel_call(body, (slots,), (main,), out)


def gathered_lower(slots, planes, main):
    rows = TILE - UPPER
    units, pieces = UPPER // rows, rows // PIECE

    def body(table, plane_table, main_ref, out_ref):
        @pl.loop(0, BLOCKS)
        def _(block):
            slot, plane = table[block], plane_table[block]

            @pl.when(slot >= 0)
            def _():
                out_ref[block] = main_ref[slot, :rows]

            @pl.when(slot < 0)
            def _():
                for part in range(pieces):
                    where = part + UPPER // PIECE
                    source = chan_of(where // CORE, plane, where % CORE)
                    out_ref[block, pl.ds(part * PIECE, PIECE)] = main_ref[source, rows:]

        @pl.loop(0, Z)
        def _(plane):
            for unit in range(units):
                for part in range(pieces):
                    where = unit * pieces + part
                    source = chan_of(where // CORE, plane, where % CORE)
                    unit_rows = pl.ds(part * PIECE, PIECE)
                    out_ref[BLOCKS + plane * units + unit, unit_rows] = main_ref[source, rows:]

    out = jax.ShapeDtypeStruct((BLOCKS + Z * units, rows, TILE), BF16)
    return kernel_call(body, (slots, planes), (main,), out)


def assembled(own_planes, partner_planes, ladder, own, partner):
    rows = TILE - UPPER
    units = UPPER // rows

    def tile_of(block, plane, upper, upper_block, lower):
        extra = BLOCKS + jnp.maximum(plane, 0) * units
        late = lower[pl.ds(extra, units)].reshape(UPPER, TILE)
        top = jnp.where(plane >= 0, late.astype(F32), upper[upper_block].astype(F32))
        return jnp.concatenate([top, lower[block].astype(F32)])

    def body(own_table, partner_table, ladder_ref, upper, lower, mirror_upper, mirror_lower, out_ref):
        i = pl.program_id(0)

        @pl.loop(0, SIDE)
        def _(j):
            cols = pl.ds(pl.multiple_of(j * TILE, TILE), TILE)
            here, there = i * SIDE + j, j * SIDE + i
            mine = tile_of(here, own_table[here], upper, j, lower)
            theirs = tile_of(there, partner_table[there], mirror_upper, there, mirror_lower)
            out_ref[:, cols] = ladder_ref[:, cols] + mine - theirs.T

    side = SIDE * TILE
    whole = [pl.BlockSpec(a.shape, lambda i: (0, 0, 0)) for a in (own[1], *partner)]
    return pl.pallas_call(
        body,
        grid=(SIDE,),
        out_shape=jax.ShapeDtypeStruct((side, side), F32),
        in_specs=[
            SMEM,
            SMEM,
            pl.BlockSpec((TILE, side), lambda i: (i, 0)),
            pl.BlockSpec((SIDE, UPPER, TILE), lambda i: (i, 0, 0)),
            *whole,
        ],
        out_specs=pl.BlockSpec((TILE, side), lambda i: (i, 0)),
        compiler_params=pltpu.CompilerParams(vmem_limit_bytes=LIMIT << 20),
    )(own_planes, partner_planes, ladder, *own, *partner)


def from_tiles(tiles):
    grid = tiles.astype(F32).reshape(SIDE, SIDE, TILE, TILE)
    return jnp.swapaxes(grid, 1, 2).reshape(SIDE * TILE, SIDE * TILE)


def pair_product(left_a, right_a, left_b, right_b):
    first = jnp.dot(left_a, right_a, preferred_element_type=F32)
    return first - jnp.dot(left_b, right_b, preferred_element_type=F32)


def ladder_term(gen_mat, ham_mat, occ_row):
    gen_occ = (gen_mat.astype(F32) * occ_row[None, :]).astype(BF16)
    ham_occ = (ham_mat.astype(F32) * occ_row[None, :]).astype(BF16)
    return pair_product(gen_occ, ham_mat, ham_occ, gen_mat)


def homes_of(owner_map):
    names = jnp.arange(CHAN, dtype=jnp.int32)
    tiles = jnp.sum((owner_map[..., None] == names).astype(jnp.int32), axis=-2)
    double = tiles == 2
    load = jnp.sum(double.astype(jnp.int32), axis=-2)
    mine, other = load[..., :, None], load[..., None, :]
    ahead = (other > mine) | ((other == mine) & (names[None, :] < names[:, None]))
    rank = jnp.sum(ahead.astype(jnp.int32), axis=-1)
    return rank, double


def on_device(generator, hamiltonian, occupation, owner, offset):
    gen_mat, ham_mat, occ_row = generator[0, 0], hamiltonian[0, 0], occupation[0, 0]
    me, grp = lax.axis_index("chan"), lax.axis_index("grp")
    my_x, my_z, my_core = me // (Z * CORE), (me // CORE) % Z, me % CORE
    owner_all = owner[:, :, :, 0]
    owners = lax.dynamic_index_in_dim(owner_all, grp, 0, keepdims=False)
    offsets = lax.dynamic_index_in_dim(offset, grp, 0, keepdims=False)
    names = jnp.arange(CHAN, dtype=jnp.int32)
    blocks = jnp.arange(BLOCKS, dtype=jnp.int32)
    steps = jnp.arange(Z, dtype=jnp.int32)

    def home_of(rank):
        row, col = rank // Z, rank % Z
        return chan_of(row // CORE, col, row % CORE)

    rank, _ = homes_of(owners)
    dest = jnp.sum(jnp.where(owners[:, :, None] == names, home_of(rank), 0), axis=-1)
    alike = (owners[:, None, :] == owners[:, :, None]) & (blocks[None, :] < blocks[:, None])
    later = jnp.any(alike, axis=-1)

    rank_all, double_all = homes_of(owner_all)
    in_plane = double_all[..., None] & ((rank_all % Z)[:, None, :, None] == steps)
    crowded = jnp.max(jnp.sum(in_plane.astype(jnp.int32), axis=2)) > 1

    my_dest = lax.dynamic_index_in_dim(dest, me, 0, keepdims=False)
    my_later = lax.dynamic_index_in_dim(later, me, 0, keepdims=False)
    my_plane = (my_dest // CORE) % Z
    to_home = my_dest[None, :] == names[:, None]
    main_blocks = jnp.max(jnp.where(to_home & ~my_later, blocks, 0), axis=1)
    direct_blocks = jnp.max(jnp.where(to_home & my_later, blocks, 0), axis=1)
    to_plane = my_plane[None, :] == ((my_z + steps) % Z)[:, None]
    second_blocks = jnp.max(jnp.where(to_plane & my_later, blocks, 0), axis=1)

    second_send = second_tiles(second_blocks, gen_mat, ham_mat)
    shifted = [z_shift(second_send[s], s) for s in range(1, Z)]
    main_send = direct_tiles(main_blocks, gen_mat, ham_mat)
    main = exchanged(main_send)
    ladder = ladder_term(gen_mat, ham_mat, occ_row)

    second_z = jnp.stack([second_send[0]] + shifted)
    same = [second_z] + [x_shift(second_z, s, 0) for s in range(1, X)]
    seconds = same + [x_shift(part, 0, 1) for part in same]

    here = dest == me
    main_place = jnp.max(jnp.where(here & ~later, offsets, -1), axis=1)
    second_place = jnp.max(jnp.where(here & later, offsets, -1), axis=1)
    flips = jnp.arange(CORE, dtype=jnp.int32)[:, None]
    shifts = jnp.arange(X, dtype=jnp.int32)[None, :]
    from_z = (my_z - steps) % Z
    came_from = chan_of(((my_x - shifts) % X)[..., None], from_z, (my_core ^ flips)[..., None]).reshape(-1)
    place_in = jnp.sum(jnp.where(came_from[:, None] == names, second_place, 0), axis=1)

    mirror = [(g, g ^ 1) for g in range(lax.axis_size("grp"))]
    slots = jnp.where(my_later, -1, my_dest)
    own_planes = jnp.where(my_later, my_plane, -1)

    def of_partner(array):
        return lax.dynamic_index_in_dim(array, grp ^ 1, 0, keepdims=False)

    named = lax.dynamic_index_in_dim(of_partner(owner_all), me, 0, keepdims=False)
    named_plane = jnp.sum(jnp.where(named[:, None] == names, of_partner(rank_all) % Z, 0), axis=-1)
    named_later = jnp.any((named[None, :] == named[:, None]) & (blocks[None, :] < blocks[:, None]), axis=-1)
    partner_planes = jnp.where(named_later, named_plane, -1)

    main, ladder, crowded, slots, own_planes, partner_planes = lax.optimization_barrier(
        (main, ladder, crowded, slots, own_planes, partner_planes)
    )
    gen_full, ham_full = placed(main_place, place_in, main, seconds)
    cross = pair_product(gen_full, ham_full, ham_full, gen_full)
    back_main_offsets = jnp.maximum(main_place, 0)

    piece_of = (((my_x + shifts) % X) * CORE + (my_core ^ flips)).reshape(-1)
    upper_send, lower_rows, *pieces = back_tiles(back_main_offsets, second_place, piece_of, cross)
    upper = exchanged(upper_send)
    routed = [
        x_shift(piece, step, flip) if step or flip else piece
        for (step, flip), piece in zip(RELATIVE, pieces)
    ]
    in_my_plane = later & ((dest // CORE) % Z == my_z)
    holder = jnp.max(jnp.where(in_my_plane, dest, 0), axis=1)
    choice = ((holder % CORE) ^ my_core) * X + (my_x - holder // (Z * CORE)) % X
    lower_send = joined(choice, lower_rows, routed)
    lower = exchanged(lower_send)

    upper_own = gathered(slots, upper)
    upper_partner = lax.ppermute(upper_own, "grp", mirror)
    lower_own = gathered_lower(slots, jnp.maximum(own_planes, 0), lower)
    lower_partner = lax.ppermute(lower_own, "grp", mirror)

    def fast():
        own, partner = (upper_own, lower_own), (upper_partner, lower_partner)
        return assembled(own_planes, partner_planes, ladder, own, partner)

    def slow():
        arrived = exchanged(direct_tiles(direct_blocks, gen_mat, ham_mat))
        gen_slow, ham_slow = placed(main_place, second_place, main, [arrived])
        cross_slow = pair_product(gen_slow, ham_slow, ham_slow, gen_slow)
        first_back = exchanged(back_direct(back_main_offsets, cross_slow))
        later_back = exchanged(back_direct(jnp.maximum(second_place, 0), cross_slow))
        back = jnp.concatenate([first_back, later_back])
        own = gathered(jnp.where(my_later, CHAN + my_dest, my_dest), back)
        partner = lax.ppermute(own, "grp", mirror)
        return ladder + from_tiles(own) - from_tiles(partner).T

    return lax.cond(crowded, slow, fast)[None, None]


def solution(mesh):
    in_specs = (
        P("grp", "chan", None, None),
        P("grp", "chan", None, None),
        P("grp", "chan", None),
        P(),
        P(),
    )
    out_specs = P("grp", "chan", None, None)

    return jax.shard_map(
        on_device, mesh=mesh, in_specs=in_specs, out_specs=out_specs, check_vma=False
    )
```

```python
import jax
import jax.numpy as jnp
from jax import lax
from jax.experimental import pallas as pl
from jax.experimental.pallas import tpu as pltpu
from jax.sharding import PartitionSpec as P


TILE = 128
SIDE = 7
BLOCKS = SIDE * SIDE
X, Z, CORE = 4, 8, 2
CHAN = X * Z * CORE
UPPER = 112
LIMIT = 24
PIECE = TILE // (X * CORE)
RELATIVE = [(step, flip) for flip in range(CORE) for step in range(X)]
F32, BF16 = jnp.float32, jnp.bfloat16


SMEM = pl.BlockSpec(memory_space=pltpu.SMEM)
VMEM = pl.BlockSpec(memory_space=pltpu.VMEM)


def chan_of(x, z, core):
    return (x * Z + z) * CORE + core


def z_shift(value, step):
    pairs = [
        (chan_of(x, z, c), chan_of(x, (z + step) % Z, c))
        for x in range(X)
        for z in range(Z)
        for c in range(CORE)
    ]
    return lax.ppermute(value, "chan", pairs)


def x_shift(value, step, flip):
    pairs = [
        (chan_of(x, z, c), chan_of((x + step) % X, z, c ^ flip))
        for x in range(X)
        for z in range(Z)
        for c in range(CORE)
    ]
    return lax.ppermute(value, "chan", pairs)


def exchanged(value):
    return lax.all_to_all(value, "chan", split_axis=0, concat_axis=0, tiled=True)


def kernel_call(body, tables, arrays, outs, scratch=(), cost=(0, 0)):
    return pl.pallas_call(
        body,
        out_shape=outs,
        in_specs=[SMEM] * len(tables) + [VMEM] * len(arrays),
        out_specs=jax.tree.map(lambda _: VMEM, outs),
        scratch_shapes=list(scratch),
        cost_estimate=pl.CostEstimate(flops=cost[0], bytes_accessed=cost[1], transcendentals=0),
        compiler_params=pltpu.CompilerParams(vmem_limit_bytes=LIMIT << 20),
    )(*tables, *arrays)


def tile_at(ref, block):
    row = pl.multiple_of((block // SIDE) * TILE, TILE)
    col = pl.multiple_of((block % SIDE) * TILE, TILE)
    return ref[pl.ds(row, TILE), pl.ds(col, TILE)]


def send_tiles(main_blocks, second_blocks, gen, ham):
    count = second_blocks.shape[0]

    def body(main_table, second_table, gen_ref, ham_ref, main_ref, *second_refs):
        for step in range(count):
            block = second_table[step]
            second_refs[step][0] = tile_at(gen_ref, block)
            second_refs[step][1] = tile_at(ham_ref, block)

        @pl.loop(0, CHAN)
        def _(slot):
            block = main_table[slot]
            main_ref[slot, 0] = tile_at(gen_ref, block)
            main_ref[slot, 1] = tile_at(ham_ref, block)

    outs = [jax.ShapeDtypeStruct((CHAN, 2, TILE, TILE), BF16)]
    outs += [jax.ShapeDtypeStruct((2, TILE, TILE), BF16)] * count
    return kernel_call(body, (main_blocks, second_blocks), (gen, ham), outs)


def direct_tiles(blocks, gen, ham):
    def body(table, gen_ref, ham_ref, out_ref):
        @pl.loop(0, CHAN)
        def _(slot):
            block = table[slot]
            out_ref[slot, 0] = tile_at(gen_ref, block)
            out_ref[slot, 1] = tile_at(ham_ref, block)

    out = jax.ShapeDtypeStruct((CHAN, 2, TILE, TILE), BF16)
    return kernel_call(body, (blocks,), (gen, ham), out)


def placed(main_offsets, second_offsets, main, seconds):
    parts = len(seconds)
    each = seconds[0].shape[0]

    def body(main_table, second_table, main_ref, *refs):
        second_refs, (gen_ref, ham_ref, total) = refs[:parts], refs[parts:]

        @pl.loop(0, BLOCKS)
        def _(block):
            total[block] = jnp.zeros((2, TILE, TILE), F32)

        @pl.loop(0, CHAN)
        def _(slot):
            place = main_table[slot]

            @pl.when(place >= 0)
            def _():
                total[place] += main_ref[slot].astype(F32)

        for part in range(parts):

            @pl.loop(0, each)
            def _(slot):
                place = second_table[part * each + slot]

                @pl.when(place >= 0)
                def _():
                    total[place] += second_refs[part][slot].astype(F32)

        @pl.loop(0, BLOCKS)
        def _(block):
            rows = pl.ds(pl.multiple_of((block // SIDE) * TILE, TILE), TILE)
            cols = pl.ds(pl.multiple_of((block % SIDE) * TILE, TILE), TILE)
            gen_ref[rows, cols] = total[block, 0].astype(BF16)
            ham_ref[rows, cols] = total[block, 1].astype(BF16)

    outs = [jax.ShapeDtypeStruct((SIDE * TILE, SIDE * TILE), BF16)] * 2
    scratch = [pltpu.VMEM((BLOCKS, 2, TILE, TILE), F32)]
    return kernel_call(body, (main_offsets, second_offsets), (main, *seconds), outs, scratch)


def back_tiles(main_offsets, second_offsets, pieces, cross):
    count = len(RELATIVE)

    def body(main_table, second_table, piece_table, cross_ref, upper_ref, lower_ref, *piece_refs):
        @pl.loop(0, CHAN)
        def _(slot):
            tile = tile_at(cross_ref, main_table[slot]).astype(BF16)
            upper_ref[slot] = tile[:UPPER]
            lower_ref[slot] = tile[UPPER:]
            block = second_table[slot]

            @pl.when(block >= 0)
            def _():
                row = (block // SIDE) * TILE
                col = pl.multiple_of((block % SIDE) * TILE, TILE)
                for part in range(count):
                    first = pl.multiple_of(row + piece_table[part] * PIECE, PIECE)
                    rows = cross_ref[pl.ds(first, PIECE), pl.ds(col, TILE)]
                    piece_refs[part][slot] = rows.astype(BF16)

    outs = [
        jax.ShapeDtypeStruct((CHAN, UPPER, TILE), BF16),
        jax.ShapeDtypeStruct((CHAN, TILE - UPPER, TILE), BF16),
    ]
    outs += [jax.ShapeDtypeStruct((CHAN, PIECE, TILE), BF16)] * count
    return kernel_call(body, (main_offsets, second_offsets, pieces), (cross,), outs)


def back_direct(main_offsets, second_offsets, cross):
    def body(main_table, second_table, cross_ref, out_ref):
        @pl.loop(0, CHAN)
        def _(slot):
            out_ref[slot, 0] = tile_at(cross_ref, main_table[slot]).astype(BF16)
            out_ref[slot, 1] = tile_at(cross_ref, second_table[slot]).astype(BF16)

    out = jax.ShapeDtypeStruct((CHAN, 2, TILE, TILE), BF16)
    return kernel_call(body, (main_offsets, second_offsets), (cross,), out)


def joined(choice, lower, routed):
    rows = TILE - UPPER

    def body(table, lower_ref, *refs):
        routed_refs, out_ref = refs[:-1], refs[-1]

        @pl.loop(0, CHAN)
        def _(slot):
            out_ref[slot, :rows] = lower_ref[slot]
            part_of = table[slot]
            for part, ref in enumerate(routed_refs):

                @pl.when(part_of == part)
                def _():
                    out_ref[slot, rows:] = ref[slot]

    out = jax.ShapeDtypeStruct((CHAN, rows + PIECE, TILE), BF16)
    return kernel_call(body, (choice,), (lower, *routed), out)


def gathered(slots, main):
    def body(table, main_ref, out_ref):
        @pl.loop(0, BLOCKS)
        def _(block):
            slot = table[block]

            @pl.when(slot >= 0)
            def _():
                out_ref[block] = main_ref[slot]

    out = jax.ShapeDtypeStruct((BLOCKS, *main.shape[1:]), BF16)
    return kernel_call(body, (slots,), (main,), out)


def in_bands(tiles):
    rows = TILE - UPPER

    def body(tile_ref, upper_ref, lower_ref):
        @pl.loop(0, BLOCKS)
        def _(block):
            tile = tile_ref[block]
            upper_ref[block] = tile[:UPPER]
            lower_ref[block] = tile[UPPER:]

    outs = [
        jax.ShapeDtypeStruct((BLOCKS, UPPER, TILE), BF16),
        jax.ShapeDtypeStruct((BLOCKS + Z * (UPPER // rows), rows, TILE), BF16),
    ]
    return kernel_call(body, (), (tiles,), outs)


def gathered_lower(slots, planes, main):
    rows = TILE - UPPER
    units, pieces = UPPER // rows, rows // PIECE

    def body(table, plane_table, main_ref, out_ref):
        @pl.loop(0, BLOCKS)
        def _(block):
            slot, plane = table[block], plane_table[block]

            @pl.when(slot >= 0)
            def _():
                out_ref[block] = main_ref[slot, :rows]

            @pl.when(slot < 0)
            def _():
                for part in range(pieces):
                    where = part + UPPER // PIECE
                    source = chan_of(where // CORE, plane, where % CORE)
                    out_ref[block, pl.ds(part * PIECE, PIECE)] = main_ref[source, rows:]

        @pl.loop(0, Z)
        def _(plane):
            for unit in range(units):
                for part in range(pieces):
                    where = unit * pieces + part
                    source = chan_of(where // CORE, plane, where % CORE)
                    unit_rows = pl.ds(part * PIECE, PIECE)
                    out_ref[BLOCKS + plane * units + unit, unit_rows] = main_ref[source, rows:]

    out = jax.ShapeDtypeStruct((BLOCKS + Z * units, rows, TILE), BF16)
    return kernel_call(body, (slots, planes), (main,), out)


def assembled(own_planes, partner_planes, ladder, own, partner):
    rows = TILE - UPPER
    units = UPPER // rows

    def tile_of(block, plane, upper, upper_block, lower):
        extra = BLOCKS + jnp.maximum(plane, 0) * units
        late = lower[pl.ds(extra, units)].reshape(UPPER, TILE)
        top = jnp.where(plane >= 0, late, upper[upper_block])
        return jnp.concatenate([top, lower[block]])

    def body(own_table, partner_table, ladder_ref, upper, lower, mirror_upper, mirror_lower, out_ref):
        i = pl.program_id(0)

        @pl.loop(0, SIDE)
        def _(j):
            cols = pl.ds(pl.multiple_of(j * TILE, TILE), TILE)
            here, there = i * SIDE + j, j * SIDE + i
            mine = tile_of(here, own_table[here], upper, j, lower)
            theirs = tile_of(there, partner_table[there], mirror_upper, there, mirror_lower)
            out_ref[:, cols] = ladder_ref[:, cols] + mine.astype(F32) - theirs.T.astype(F32)

    side = SIDE * TILE
    whole = [pl.BlockSpec(a.shape, lambda i: (0, 0, 0)) for a in (own[1], *partner)]
    return pl.pallas_call(
        body,
        grid=(SIDE,),
        out_shape=jax.ShapeDtypeStruct((side, side), F32),
        in_specs=[
            SMEM,
            SMEM,
            pl.BlockSpec((TILE, side), lambda i: (i, 0)),
            pl.BlockSpec((SIDE, UPPER, TILE), lambda i: (i, 0, 0)),
            *whole,
        ],
        out_specs=pl.BlockSpec((TILE, side), lambda i: (i, 0)),
        compiler_params=pltpu.CompilerParams(vmem_limit_bytes=LIMIT << 20),
    )(own_planes, partner_planes, ladder, *own, *partner)


def pair_product(left_a, right_a, left_b, right_b):
    first = jnp.dot(left_a, right_a, preferred_element_type=F32)
    return first - jnp.dot(left_b, right_b, preferred_element_type=F32)


def commutator_by_rows(gen, ham):
    def body(gen_rows, ham_rows, gen_ref, ham_ref, out_ref):
        first = jnp.dot(gen_rows[...], ham_ref[...], preferred_element_type=F32)
        out_ref[...] = first - jnp.dot(ham_rows[...], gen_ref[...], preferred_element_type=F32)

    band = pl.BlockSpec((TILE, SIDE * TILE), lambda i: (i, 0))
    whole = pl.BlockSpec(gen.shape, lambda i: (0, 0))
    return pl.pallas_call(
        body,
        grid=(SIDE,),
        out_shape=jax.ShapeDtypeStruct(gen.shape, F32),
        in_specs=[band, band, whole, whole],
        out_specs=band,
        compiler_params=pltpu.CompilerParams(vmem_limit_bytes=LIMIT << 20),
    )(gen, ham, gen, ham)


def ladder_term(gen_mat, ham_mat, occ_row):
    gen_occ = (gen_mat.astype(F32) * occ_row[None, :]).astype(BF16)
    ham_occ = (ham_mat.astype(F32) * occ_row[None, :]).astype(BF16)
    return pair_product(gen_occ, ham_mat, ham_occ, gen_mat)


def homes_of(owner_map):
    names = jnp.arange(CHAN, dtype=jnp.int32)
    tiles = jnp.sum((owner_map[..., None] == names).astype(jnp.int32), axis=-2)
    double = tiles == 2
    load = jnp.sum(double.astype(jnp.int32), axis=-2)
    mine, other = load[..., :, None], load[..., None, :]
    ahead = (other > mine) | ((other == mine) & (names[None, :] < names[:, None]))
    rank = jnp.sum(ahead.astype(jnp.int32), axis=-1)
    return rank, double


def on_device(generator, hamiltonian, occupation, owner, offset):
    gen_mat, ham_mat, occ_row = generator[0, 0], hamiltonian[0, 0], occupation[0, 0]
    me, grp = lax.axis_index("chan"), lax.axis_index("grp")
    my_x, my_z, my_core = me // (Z * CORE), (me // CORE) % Z, me % CORE
    owner_all = owner[:, :, :, 0]
    owners = lax.dynamic_index_in_dim(owner_all, grp, 0, keepdims=False)
    offsets = lax.dynamic_index_in_dim(offset, grp, 0, keepdims=False)
    names = jnp.arange(CHAN, dtype=jnp.int32)
    blocks = jnp.arange(BLOCKS, dtype=jnp.int32)
    steps = jnp.arange(Z, dtype=jnp.int32)

    def home_of(rank):
        row, col = rank // Z, rank % Z
        return chan_of(row // CORE, col, row % CORE)

    rank, _ = homes_of(owners)
    dest = jnp.sum(jnp.where(owners[:, :, None] == names, home_of(rank), 0), axis=-1)
    alike = (owners[:, None, :] == owners[:, :, None]) & (blocks[None, :] < blocks[:, None])
    later = jnp.any(alike, axis=-1)

    my_dest = lax.dynamic_index_in_dim(dest, me, 0, keepdims=False)
    my_later = lax.dynamic_index_in_dim(later, me, 0, keepdims=False)
    my_plane = (my_dest // CORE) % Z
    to_home = my_dest[None, :] == names[:, None]
    main_blocks = jnp.max(jnp.where(to_home & ~my_later, blocks, 0), axis=1)
    direct_blocks = jnp.max(jnp.where(to_home & my_later, blocks, 0), axis=1)
    to_plane = my_plane[None, :] == ((my_z + steps) % Z)[:, None]
    second_blocks = jnp.max(jnp.where(to_plane & my_later, blocks, 0), axis=1)

    main_send, *second_send = send_tiles(main_blocks, second_blocks, gen_mat, ham_mat)
    second_send[0], owner_late = lax.optimization_barrier((second_send[0], owner_all))
    rank_all, double_all = homes_of(owner_late)
    planes_all = ((rank_all % Z)[..., None] == steps).astype(BF16)
    in_plane = jnp.einsum("gck,gkt->gct", double_all.astype(BF16), planes_all, preferred_element_type=F32)
    crowded = jnp.max(in_plane) > 1.5

    shifted = [z_shift(second_send[s], s) for s in range(1, Z)]
    main = exchanged(main_send)
    ladder = ladder_term(gen_mat, ham_mat, occ_row)

    second_z = jnp.stack([second_send[0]] + shifted)
    same = [second_z] + [x_shift(second_z, s, 0) for s in range(1, X)]
    seconds = same + [x_shift(part, 0, 1) for part in same]

    here = dest == me
    main_place = jnp.max(jnp.where(here & ~later, offsets, -1), axis=1)
    second_place = jnp.max(jnp.where(here & later, offsets, -1), axis=1)
    flips = jnp.arange(CORE, dtype=jnp.int32)[:, None]
    shifts = jnp.arange(X, dtype=jnp.int32)[None, :]
    from_z = (my_z - steps) % Z
    came_from = chan_of(((my_x - shifts) % X)[..., None], from_z, (my_core ^ flips)[..., None]).reshape(-1)
    place_in = jnp.sum(jnp.where(came_from[:, None] == names, second_place, 0), axis=1)

    mirror = [(g, g ^ 1) for g in range(lax.axis_size("grp"))]
    slots = jnp.where(my_later, -1, my_dest)
    own_planes = jnp.where(my_later, my_plane, -1)

    def of_partner(array):
        return lax.dynamic_index_in_dim(array, grp ^ 1, 0, keepdims=False)

    named = lax.dynamic_index_in_dim(of_partner(owner_late), me, 0, keepdims=False)
    named_one = (named[:, None] == names).astype(BF16)
    named_plane = jnp.dot(named_one, of_partner(planes_all), preferred_element_type=F32)
    named_plane = jnp.sum(named_plane.astype(jnp.int32) * steps, axis=-1)
    named_later = jnp.any((named[None, :] == named[:, None]) & (blocks[None, :] < blocks[:, None]), axis=-1)
    partner_planes = jnp.where(named_later, named_plane, -1)

    main, ladder, crowded, slots, own_planes, partner_planes = lax.optimization_barrier(
        (main, ladder, crowded, slots, own_planes, partner_planes)
    )
    gen_full, ham_full = placed(main_place, place_in, main, seconds)
    cross = pair_product(gen_full, ham_full, ham_full, gen_full)
    back_main_offsets = jnp.maximum(main_place, 0)

    piece_of = (((my_x + shifts) % X) * CORE + (my_core ^ flips)).reshape(-1)
    upper_send, lower_rows, *pieces = back_tiles(back_main_offsets, second_place, piece_of, cross)
    upper = exchanged(upper_send)
    routed = [
        x_shift(piece, step, flip) if step or flip else piece
        for (step, flip), piece in zip(RELATIVE, pieces)
    ]
    in_my_plane = later & ((dest // CORE) % Z == my_z)
    holder = jnp.max(jnp.where(in_my_plane, dest, 0), axis=1)
    choice = ((holder % CORE) ^ my_core) * X + (my_x - holder // (Z * CORE)) % X
    lower_send = joined(choice, lower_rows, routed)
    lower = exchanged(lower_send)

    upper_own = gathered(slots, upper)
    upper_partner = lax.ppermute(upper_own, "grp", mirror)
    lower_own = gathered_lower(slots, jnp.maximum(own_planes, 0), lower)
    lower_partner = lax.ppermute(lower_own, "grp", mirror)

    def fast():
        own, partner = (upper_own, lower_own), (upper_partner, lower_partner)
        return assembled(own_planes, partner_planes, ladder, own, partner)

    def slow():
        arrived = exchanged(direct_tiles(direct_blocks, gen_mat, ham_mat))
        gen_slow, ham_slow = placed(main_place, second_place, main, [arrived])
        cross_slow = commutator_by_rows(gen_slow, ham_slow)
        back = exchanged(back_direct(back_main_offsets, jnp.maximum(second_place, 0), cross_slow))
        back = back.reshape(2 * CHAN, TILE, TILE)
        own = gathered(2 * my_dest + my_later.astype(jnp.int32), back)
        partner = in_bands(lax.ppermute(own, "grp", mirror))
        nowhere = jnp.full((BLOCKS,), -1, jnp.int32)
        return assembled(nowhere, nowhere, ladder, in_bands(own), partner)

    return lax.cond(crowded, slow, fast)[None, None]


def solution(mesh):
    in_specs = (
        P("grp", "chan", None, None),
        P("grp", "chan", None, None),
        P("grp", "chan", None),
        P(),
        P(),
    )
    out_specs = P("grp", "chan", None, None)

    return jax.shard_map(
        on_device, mesh=mesh, in_specs=in_specs, out_specs=out_specs, check_vma=False
    )
```

```python
import jax
import jax.numpy as jnp
from jax import lax
from jax.experimental import pallas as pl
from jax.experimental.pallas import tpu as pltpu
from jax.sharding import PartitionSpec as P


TILE = 128
SIDE = 7
BLOCKS = SIDE * SIDE
X, Z, CORE = 4, 8, 2
CHAN = X * Z * CORE
UPPER = 112
LIMIT = 24
PIECE = TILE // (X * CORE)
RELATIVE = [(step, flip) for flip in range(CORE) for step in range(X)]
F32, BF16 = jnp.float32, jnp.bfloat16


SMEM = pl.BlockSpec(memory_space=pltpu.SMEM)
VMEM = pl.BlockSpec(memory_space=pltpu.VMEM)
HBM = pl.BlockSpec(memory_space=pltpu.HBM)
CHUNKS = 4


def chan_of(x, z, core):
    return (x * Z + z) * CORE + core


def z_shift(value, step):
    pairs = [
        (chan_of(x, z, c), chan_of(x, (z + step) % Z, c))
        for x in range(X)
        for z in range(Z)
        for c in range(CORE)
    ]
    return lax.ppermute(value, "chan", pairs)


def x_shift(value, step, flip):
    pairs = [
        (chan_of(x, z, c), chan_of((x + step) % X, z, c ^ flip))
        for x in range(X)
        for z in range(Z)
        for c in range(CORE)
    ]
    return lax.ppermute(value, "chan", pairs)


def exchanged(value):
    return lax.all_to_all(value, "chan", split_axis=0, concat_axis=0, tiled=True)


def kernel_call(body, tables, arrays, outs, scratch=(), far_in=0, far_out=0):
    out_specs = VMEM
    if isinstance(outs, list):
        out_specs = [HBM] * far_out + [VMEM] * (len(outs) - far_out)
    return pl.pallas_call(
        body,
        out_shape=outs,
        in_specs=[SMEM] * len(tables) + [HBM] * far_in + [VMEM] * (len(arrays) - far_in),
        out_specs=out_specs,
        scratch_shapes=list(scratch),
        compiler_params=pltpu.CompilerParams(vmem_limit_bytes=LIMIT << 20),
    )(*tables, *arrays)


def tile_at(ref, block):
    row = pl.multiple_of((block // SIDE) * TILE, TILE)
    col = pl.multiple_of((block % SIDE) * TILE, TILE)
    return ref[pl.ds(row, TILE), pl.ds(col, TILE)]


def send_tiles(main_blocks, second_blocks, gen, ham):
    count = second_blocks.shape[0]
    chunk = CHAN // CHUNKS

    def body(main_table, second_table, gen_ref, ham_ref, main_ref, *refs):
        second_refs, (held, done) = refs[:count], refs[count:]
        copies = []
        for part in range(CHUNKS):

            @pl.loop(part * chunk, (part + 1) * chunk)
            def _(slot):
                block = main_table[slot]
                held[slot, 0] = tile_at(gen_ref, block)
                held[slot, 1] = tile_at(ham_ref, block)

            where = pl.ds(part * chunk, chunk)
            copies.append(pltpu.make_async_copy(held.at[where], main_ref.at[where], done.at[part]))
            copies[-1].start()
        for step in range(count):
            block = second_table[step]
            second_refs[step][0] = tile_at(gen_ref, block)
            second_refs[step][1] = tile_at(ham_ref, block)
        for copy in copies:
            copy.wait()

    outs = [pltpu.HBM((CHAN, 2, TILE, TILE), BF16)]
    scratch = [pltpu.VMEM(outs[0].shape, BF16), pltpu.SemaphoreType.DMA((CHUNKS,))]
    outs += [jax.ShapeDtypeStruct((2, TILE, TILE), BF16)] * count
    return kernel_call(body, (main_blocks, second_blocks), (gen, ham), outs, scratch, far_out=1)


def direct_tiles(blocks, gen, ham):
    def body(table, gen_ref, ham_ref, out_ref):
        @pl.loop(0, CHAN)
        def _(slot):
            block = table[slot]
            out_ref[slot, 0] = tile_at(gen_ref, block)
            out_ref[slot, 1] = tile_at(ham_ref, block)

    out = jax.ShapeDtypeStruct((CHAN, 2, TILE, TILE), BF16)
    return kernel_call(body, (blocks,), (gen, ham), out)


def placed(main_offsets, second_offsets, main, seconds):
    parts = len(seconds)
    each = seconds[0].shape[0]
    chunk = CHAN // CHUNKS

    def body(main_table, second_table, main_ref, *refs):
        second_refs, (gen_ref, ham_ref, total, held, done) = refs[:parts], refs[parts:]
        copies = []
        for part in range(CHUNKS):
            where = pl.ds(part * chunk, chunk)
            copies.append(pltpu.make_async_copy(main_ref.at[where], held.at[where], done.at[part]))
            copies[-1].start()

        @pl.loop(0, BLOCKS)
        def _(block):
            total[block] = jnp.zeros((2, TILE, TILE), F32)

        for part in range(parts):

            @pl.loop(0, each)
            def _(slot):
                place = second_table[part * each + slot]

                @pl.when(place >= 0)
                def _():
                    total[place] += second_refs[part][slot].astype(F32)

        for part in range(CHUNKS):
            copies[part].wait()

            @pl.loop(part * chunk, (part + 1) * chunk)
            def _(slot):
                place = main_table[slot]

                @pl.when(place >= 0)
                def _():
                    total[place] += held[slot].astype(F32)

        @pl.loop(0, BLOCKS)
        def _(block):
            rows = pl.ds(pl.multiple_of((block // SIDE) * TILE, TILE), TILE)
            cols = pl.ds(pl.multiple_of((block % SIDE) * TILE, TILE), TILE)
            gen_ref[rows, cols] = total[block, 0].astype(BF16)
            ham_ref[rows, cols] = total[block, 1].astype(BF16)

    outs = [jax.ShapeDtypeStruct((SIDE * TILE, SIDE * TILE), BF16)] * 2
    scratch = [
        pltpu.VMEM((BLOCKS, 2, TILE, TILE), F32),
        pltpu.VMEM(main.shape, BF16),
        pltpu.SemaphoreType.DMA((CHUNKS,)),
    ]
    tables, arrays = (main_offsets, second_offsets), (main, *seconds)
    return kernel_call(body, tables, arrays, outs, scratch, far_in=1)


def back_tiles(main_offsets, second_offsets, pieces, cross):
    count = len(RELATIVE)

    chunk = CHAN // CHUNKS

    def body(main_table, second_table, piece_table, cross_ref, upper_ref, lower_ref, *refs):
        piece_refs, (held, done) = refs[:count], refs[count:]
        copies = []
        for part in range(CHUNKS):

            @pl.loop(part * chunk, (part + 1) * chunk)
            def _(slot):
                tile = tile_at(cross_ref, main_table[slot]).astype(BF16)
                held[slot] = tile[:UPPER]
                lower_ref[slot] = tile[UPPER:]

            where = pl.ds(part * chunk, chunk)
            copies.append(pltpu.make_async_copy(held.at[where], upper_ref.at[where], done.at[part]))
            copies[-1].start()

        @pl.loop(0, CHAN)
        def _(slot):
            block = second_table[slot]

            @pl.when(block >= 0)
            def _():
                row = (block // SIDE) * TILE
                col = pl.multiple_of((block % SIDE) * TILE, TILE)
                for part in range(count):
                    first = pl.multiple_of(row + piece_table[part] * PIECE, PIECE)
                    rows = cross_ref[pl.ds(first, PIECE), pl.ds(col, TILE)]
                    piece_refs[part][slot] = rows.astype(BF16)

        for copy in copies:
            copy.wait()

    outs = [
        pltpu.HBM((CHAN, UPPER, TILE), BF16),
        jax.ShapeDtypeStruct((CHAN, TILE - UPPER, TILE), BF16),
    ]
    scratch = [pltpu.VMEM(outs[0].shape, BF16), pltpu.SemaphoreType.DMA((CHUNKS,))]
    outs += [jax.ShapeDtypeStruct((CHAN, PIECE, TILE), BF16)] * count
    tables = (main_offsets, second_offsets, pieces)
    return kernel_call(body, tables, (cross,), outs, scratch, far_out=1)


def back_direct(main_offsets, second_offsets, cross):
    def body(main_table, second_table, cross_ref, out_ref):
        @pl.loop(0, CHAN)
        def _(slot):
            out_ref[slot, 0] = tile_at(cross_ref, main_table[slot]).astype(BF16)
            out_ref[slot, 1] = tile_at(cross_ref, second_table[slot]).astype(BF16)

    out = jax.ShapeDtypeStruct((CHAN, 2, TILE, TILE), BF16)
    return kernel_call(body, (main_offsets, second_offsets), (cross,), out)


def joined(choice, lower, routed):
    rows, parts = TILE - UPPER, len(routed)

    def body(table, lower_ref, *refs):
        routed_refs, (out_ref, held) = refs[:parts], refs[parts:]

        @pl.loop(0, CHAN)
        def _(slot):
            for part in range(parts):
                held[part, slot] = routed_refs[part][slot]

        @pl.loop(0, CHAN)
        def _(slot):
            out_ref[slot, :rows] = lower_ref[slot]
            out_ref[slot, rows:] = held[table[slot], slot]

    out = pltpu.HBM((CHAN, rows + PIECE, TILE), BF16)
    scratch = [pltpu.VMEM((parts, CHAN, PIECE, TILE), BF16)]
    return kernel_call(body, (choice,), (lower, *routed), out, scratch)


def gathered(slots, main):
    def body(table, main_ref, out_ref):
        @pl.loop(0, BLOCKS)
        def _(block):
            slot = table[block]

            @pl.when(slot >= 0)
            def _():
                out_ref[block] = main_ref[slot]

    out = jax.ShapeDtypeStruct((BLOCKS, *main.shape[1:]), BF16)
    return kernel_call(body, (slots,), (main,), out)


def in_bands(tiles):
    rows = TILE - UPPER

    def body(tile_ref, upper_ref, lower_ref):
        @pl.loop(0, BLOCKS)
        def _(block):
            tile = tile_ref[block]
            upper_ref[block] = tile[:UPPER]
            lower_ref[block] = tile[UPPER:]

    outs = [
        jax.ShapeDtypeStruct((BLOCKS, UPPER, TILE), BF16),
        jax.ShapeDtypeStruct((BLOCKS + Z * (UPPER // rows), rows, TILE), BF16),
    ]
    return kernel_call(body, (), (tiles,), outs)


def gathered_lower(slots, planes, main):
    rows = TILE - UPPER
    units, pieces = UPPER // rows, rows // PIECE

    def body(table, plane_table, main_ref, out_ref):
        @pl.loop(0, BLOCKS)
        def _(block):
            slot, plane = table[block], plane_table[block]

            @pl.when(slot >= 0)
            def _():
                out_ref[block] = main_ref[slot, :rows]

            @pl.when(slot < 0)
            def _():
                for part in range(pieces):
                    where = part + UPPER // PIECE
                    source = chan_of(where // CORE, plane, where % CORE)
                    out_ref[block, pl.ds(part * PIECE, PIECE)] = main_ref[source, rows:]

        @pl.loop(0, Z)
        def _(plane):
            for unit in range(units):
                for part in range(pieces):
                    where = unit * pieces + part
                    source = chan_of(where // CORE, plane, where % CORE)
                    unit_rows = pl.ds(part * PIECE, PIECE)
                    out_ref[BLOCKS + plane * units + unit, unit_rows] = main_ref[source, rows:]

    out = jax.ShapeDtypeStruct((BLOCKS + Z * units, rows, TILE), BF16)
    return kernel_call(body, (slots, planes), (main,), out)


def whole_tile(block, plane, upper, upper_block, lower):
    units = UPPER // (TILE - UPPER)
    late = lower[pl.ds(BLOCKS + jnp.maximum(plane, 0) * units, units)].reshape(UPPER, TILE)
    top = jnp.where(plane >= 0, late, upper[upper_block])
    return jnp.concatenate([top, lower[block]])


def by_bands(body, table, full, upper, upper_spec, lower, kind):
    side = SIDE * TILE
    band = pl.BlockSpec((TILE, side), lambda i: (i, 0))
    return pl.pallas_call(
        body,
        grid=(SIDE,),
        out_shape=kind((side, side), F32),
        in_specs=[SMEM, band, upper_spec, pl.BlockSpec(lower.shape, lambda i: (0, 0, 0))],
        out_specs=band,
        compiler_params=pltpu.CompilerParams(vmem_limit_bytes=12 << 20),
    )(table, full, upper, lower)


def plus_own(planes, ladder, upper, lower):
    def body(table, ladder_ref, upper_ref, lower_ref, out_ref):
        i = pl.program_id(0)

        @pl.loop(0, SIDE)
        def _(j):
            cols = pl.ds(pl.multiple_of(j * TILE, TILE), TILE)
            block = i * SIDE + j
            tile = whole_tile(block, table[block], upper_ref, j, lower_ref)
            out_ref[:, cols] = ladder_ref[:, cols] + tile.astype(F32)

    upper_spec = pl.BlockSpec((SIDE, UPPER, TILE), lambda i: (i, 0, 0))
    return by_bands(body, planes, ladder, upper, upper_spec, lower, jax.ShapeDtypeStruct)


def minus_mirror(planes, base, upper, lower):
    def body(table, base_ref, upper_ref, lower_ref, out_ref):
        i = pl.program_id(0)

        @pl.loop(0, SIDE)
        def _(j):
            cols = pl.ds(pl.multiple_of(j * TILE, TILE), TILE)
            block = j * SIDE + i
            tile = whole_tile(block, table[block], upper_ref, block, lower_ref)
            out_ref[:, cols] = base_ref[:, cols] - tile.T.astype(F32)

    upper_spec = pl.BlockSpec(upper.shape, lambda i: (0, 0, 0))
    return by_bands(body, planes, base, upper, upper_spec, lower, pltpu.HBM)


def pair_product(left_a, right_a, left_b, right_b):
    first = jnp.dot(left_a, right_a, preferred_element_type=F32)
    return first - jnp.dot(left_b, right_b, preferred_element_type=F32)


def commutator_by_rows(gen, ham):
    def body(gen_rows, ham_rows, gen_ref, ham_ref, out_ref):
        first = jnp.dot(gen_rows[...], ham_ref[...], preferred_element_type=F32)
        out_ref[...] = first - jnp.dot(ham_rows[...], gen_ref[...], preferred_element_type=F32)

    band = pl.BlockSpec((TILE, SIDE * TILE), lambda i: (i, 0))
    whole = pl.BlockSpec(gen.shape, lambda i: (0, 0))
    return pl.pallas_call(
        body,
        grid=(SIDE,),
        out_shape=jax.ShapeDtypeStruct(gen.shape, F32),
        in_specs=[band, band, whole, whole],
        out_specs=band,
        compiler_params=pltpu.CompilerParams(vmem_limit_bytes=LIMIT << 20),
    )(gen, ham, gen, ham)


def ladder_term(gen_mat, ham_mat, occ_row):
    gen_occ = (gen_mat.astype(F32) * occ_row[None, :]).astype(BF16)
    ham_occ = (ham_mat.astype(F32) * occ_row[None, :]).astype(BF16)
    return pair_product(gen_occ, ham_mat, ham_occ, gen_mat)


def homes_of(owner_map):
    names = jnp.arange(CHAN, dtype=jnp.int32)
    tiles = jnp.sum((owner_map[..., None] == names).astype(jnp.int32), axis=-2)
    double = tiles == 2
    load = jnp.sum(double.astype(jnp.int32), axis=-2)
    mine, other = load[..., :, None], load[..., None, :]
    ahead = (other > mine) | ((other == mine) & (names[None, :] < names[:, None]))
    rank = jnp.sum(ahead.astype(jnp.int32), axis=-1)
    return rank, double


def on_device(generator, hamiltonian, occupation, owner, offset):
    gen_mat, ham_mat, occ_row = generator[0, 0], hamiltonian[0, 0], occupation[0, 0]
    me, grp = lax.axis_index("chan"), lax.axis_index("grp")
    my_x, my_z, my_core = me // (Z * CORE), (me // CORE) % Z, me % CORE
    owner_all = owner[:, :, :, 0]
    owners = lax.dynamic_index_in_dim(owner_all, grp, 0, keepdims=False)
    offsets = lax.dynamic_index_in_dim(offset, grp, 0, keepdims=False)
    names = jnp.arange(CHAN, dtype=jnp.int32)
    blocks = jnp.arange(BLOCKS, dtype=jnp.int32)
    steps = jnp.arange(Z, dtype=jnp.int32)

    def home_of(rank):
        row, col = rank // Z, rank % Z
        return chan_of(row // CORE, col, row % CORE)

    rank, _ = homes_of(owners)
    dest = jnp.sum(jnp.where(owners[:, :, None] == names, home_of(rank), 0), axis=-1)
    alike = (owners[:, None, :] == owners[:, :, None]) & (blocks[None, :] < blocks[:, None])
    later = jnp.any(alike, axis=-1)

    my_dest = lax.dynamic_index_in_dim(dest, me, 0, keepdims=False)
    my_later = lax.dynamic_index_in_dim(later, me, 0, keepdims=False)
    my_plane = (my_dest // CORE) % Z
    to_home = my_dest[None, :] == names[:, None]
    main_blocks = jnp.max(jnp.where(to_home & ~my_later, blocks, 0), axis=1)
    direct_blocks = jnp.max(jnp.where(to_home & my_later, blocks, 0), axis=1)
    to_plane = my_plane[None, :] == ((my_z + steps) % Z)[:, None]
    second_blocks = jnp.max(jnp.where(to_plane & my_later, blocks, 0), axis=1)

    main_send, *second_send = send_tiles(main_blocks, second_blocks, gen_mat, ham_mat)
    second_send[0], owner_late = lax.optimization_barrier((second_send[0], owner_all))
    rank_all, double_all = homes_of(owner_late)
    planes_all = ((rank_all % Z)[..., None] == steps).astype(BF16)
    in_plane = jnp.einsum("gck,gkt->gct", double_all.astype(BF16), planes_all, preferred_element_type=F32)
    crowded = jnp.max(in_plane) > 1.5

    shifted = [z_shift(second_send[s], s) for s in range(1, Z)]
    main = exchanged(main_send)
    ladder = ladder_term(gen_mat, ham_mat, occ_row)

    second_z = jnp.stack([second_send[0]] + shifted)
    same = [second_z] + [x_shift(second_z, s, 0) for s in range(1, X)]
    seconds = same + [x_shift(part, 0, 1) for part in same]

    here = dest == me
    main_place = jnp.max(jnp.where(here & ~later, offsets, -1), axis=1)
    second_place = jnp.max(jnp.where(here & later, offsets, -1), axis=1)
    flips = jnp.arange(CORE, dtype=jnp.int32)[:, None]
    shifts = jnp.arange(X, dtype=jnp.int32)[None, :]
    from_z = (my_z - steps) % Z
    came_from = chan_of(((my_x - shifts) % X)[..., None], from_z, (my_core ^ flips)[..., None]).reshape(-1)
    place_in = jnp.sum(jnp.where(came_from[:, None] == names, second_place, 0), axis=1)

    mirror = [(g, g ^ 1) for g in range(lax.axis_size("grp"))]
    slots = jnp.where(my_later, -1, my_dest)
    own_planes = jnp.where(my_later, my_plane, -1)

    def of_partner(array):
        return lax.dynamic_index_in_dim(array, grp ^ 1, 0, keepdims=False)

    named = lax.dynamic_index_in_dim(of_partner(owner_late), me, 0, keepdims=False)
    named_one = (named[:, None] == names).astype(BF16)
    named_plane = jnp.dot(named_one, of_partner(planes_all), preferred_element_type=F32)
    named_plane = jnp.sum(named_plane.astype(jnp.int32) * steps, axis=-1)
    named_later = jnp.any((named[None, :] == named[:, None]) & (blocks[None, :] < blocks[:, None]), axis=-1)
    partner_planes = jnp.where(named_later, named_plane, -1)

    main, ladder, crowded, slots, own_planes, partner_planes = lax.optimization_barrier(
        (main, ladder, crowded, slots, own_planes, partner_planes)
    )
    gen_full, ham_full = placed(main_place, place_in, main, seconds)
    cross = pair_product(gen_full, ham_full, ham_full, gen_full)
    back_main_offsets = jnp.maximum(main_place, 0)

    piece_of = (((my_x + shifts) % X) * CORE + (my_core ^ flips)).reshape(-1)
    upper_send, lower_rows, *pieces = back_tiles(back_main_offsets, second_place, piece_of, cross)
    upper = exchanged(upper_send)
    routed = [
        x_shift(piece, step, flip) if step or flip else piece
        for (step, flip), piece in zip(RELATIVE, pieces)
    ]
    in_my_plane = later & ((dest // CORE) % Z == my_z)
    holder = jnp.max(jnp.where(in_my_plane, dest, 0), axis=1)
    choice = ((holder % CORE) ^ my_core) * X + (my_x - holder // (Z * CORE)) % X
    lower_send = joined(choice, lower_rows, routed)
    lower = exchanged(lower_send)

    upper_own = gathered(slots, upper)
    upper_partner = lax.ppermute(upper_own, "grp", mirror)
    lower_own = gathered_lower(slots, jnp.maximum(own_planes, 0), lower)
    lower_partner = lax.ppermute(lower_own, "grp", mirror)

    base = plus_own(own_planes, ladder, upper_own, lower_own)

    def fast():
        return minus_mirror(partner_planes, base, upper_partner, lower_partner)

    def slow():
        arrived = exchanged(direct_tiles(direct_blocks, gen_mat, ham_mat))
        gen_slow, ham_slow = placed(main_place, second_place, main, [arrived])
        cross_slow = commutator_by_rows(gen_slow, ham_slow)
        back = exchanged(back_direct(back_main_offsets, jnp.maximum(second_place, 0), cross_slow))
        back = back.reshape(2 * CHAN, TILE, TILE)
        own = gathered(2 * my_dest + my_later.astype(jnp.int32), back)
        partner = in_bands(lax.ppermute(own, "grp", mirror))
        nowhere = jnp.full((BLOCKS,), -1, jnp.int32)
        return minus_mirror(nowhere, plus_own(nowhere, ladder, *in_bands(own)), *partner)

    return lax.cond(crowded, slow, fast)[None, None]


def solution(mesh):
    in_specs = (
        P("grp", "chan", None, None),
        P("grp", "chan", None, None),
        P("grp", "chan", None),
        P(),
        P(),
    )
    out_specs = P("grp", "chan", None, None)

    return jax.shard_map(
        on_device, mesh=mesh, in_specs=in_specs, out_specs=out_specs, check_vma=False
    )
```

```python
import jax
import jax.numpy as jnp
from jax import lax
from jax.experimental import pallas as pl
from jax.experimental.pallas import tpu as pltpu
from jax.sharding import PartitionSpec as P


TILE = 128
SIDE = 7
BLOCKS = SIDE * SIDE
X, Z, CORE = 4, 8, 2
CHAN = X * Z * CORE
UPPER = 112
LIMIT = 24
PIECE = TILE // (X * CORE)
HOPS = (0, 4, 3, 5, 2, 6, 1, 7)
RELATIVE = [(step, flip) for flip in range(CORE) for step in range(X)]
F32, BF16 = jnp.float32, jnp.bfloat16


SMEM = pl.BlockSpec(memory_space=pltpu.SMEM)
VMEM = pl.BlockSpec(memory_space=pltpu.VMEM)
HBM = pl.BlockSpec(memory_space=pltpu.HBM)
CHUNKS = 4


def chan_of(x, z, core):
    return (x * Z + z) * CORE + core


def z_shift(value, step):
    pairs = [
        (chan_of(x, z, c), chan_of(x, (z + step) % Z, c))
        for x in range(X)
        for z in range(Z)
        for c in range(CORE)
    ]
    return lax.ppermute(value, "chan", pairs)


def x_shift(value, step, flip):
    pairs = [
        (chan_of(x, z, c), chan_of((x + step) % X, z, c ^ flip))
        for x in range(X)
        for z in range(Z)
        for c in range(CORE)
    ]
    return lax.ppermute(value, "chan", pairs)


def exchanged(value):
    return lax.all_to_all(value, "chan", split_axis=0, concat_axis=0, tiled=True)


def kernel_call(body, tables, arrays, outs, scratch=(), far_in=0, far_out=0):
    out_specs = VMEM
    if isinstance(outs, list):
        out_specs = [HBM] * far_out + [VMEM] * (len(outs) - far_out)
    return pl.pallas_call(
        body,
        out_shape=outs,
        in_specs=[SMEM] * len(tables) + [HBM] * far_in + [VMEM] * (len(arrays) - far_in),
        out_specs=out_specs,
        scratch_shapes=list(scratch),
        compiler_params=pltpu.CompilerParams(vmem_limit_bytes=LIMIT << 20),
    )(*tables, *arrays)


def tile_at(ref, block):
    row = pl.multiple_of((block // SIDE) * TILE, TILE)
    col = pl.multiple_of((block % SIDE) * TILE, TILE)
    return ref[pl.ds(row, TILE), pl.ds(col, TILE)]


def send_tiles(main_blocks, second_blocks, gen, ham):
    count = second_blocks.shape[0]
    chunk = CHAN // CHUNKS

    def body(main_table, second_table, gen_ref, ham_ref, main_ref, *refs):
        second_refs, (held, done) = refs[:count], refs[count:]
        copies = []
        for part in range(CHUNKS):

            @pl.loop(part * chunk, (part + 1) * chunk)
            def _(slot):
                block = main_table[slot]
                held[slot, 0] = tile_at(gen_ref, block)
                held[slot, 1] = tile_at(ham_ref, block)

            where = pl.ds(part * chunk, chunk)
            copies.append(pltpu.make_async_copy(held.at[where], main_ref.at[where], done.at[part]))
            copies[-1].start()
        for step in range(count):
            block = second_table[step]
            second_refs[step][0] = tile_at(gen_ref, block)
            second_refs[step][1] = tile_at(ham_ref, block)
        for copy in copies:
            copy.wait()

    outs = [pltpu.HBM((CHAN, 2, TILE, TILE), BF16)]
    scratch = [pltpu.VMEM(outs[0].shape, BF16), pltpu.SemaphoreType.DMA((CHUNKS,))]
    outs += [jax.ShapeDtypeStruct((2, TILE, TILE), BF16)] * count
    return kernel_call(body, (main_blocks, second_blocks), (gen, ham), outs, scratch, far_out=1)


def direct_tiles(blocks, gen, ham):
    def body(table, gen_ref, ham_ref, out_ref):
        @pl.loop(0, CHAN)
        def _(slot):
            block = table[slot]
            out_ref[slot, 0] = tile_at(gen_ref, block)
            out_ref[slot, 1] = tile_at(ham_ref, block)

    out = jax.ShapeDtypeStruct((CHAN, 2, TILE, TILE), BF16)
    return kernel_call(body, (blocks,), (gen, ham), out)


def placed(main_offsets, second_offsets, main, seconds):
    parts = len(seconds)
    each = seconds[0].shape[0]
    chunk = CHAN // CHUNKS

    def body(main_table, second_table, main_ref, *refs):
        second_refs, (gen_ref, ham_ref, total, held, done) = refs[:parts], refs[parts:]
        copies = []
        for part in range(CHUNKS):
            where = pl.ds(part * chunk, chunk)
            copies.append(pltpu.make_async_copy(main_ref.at[where], held.at[where], done.at[part]))
            copies[-1].start()

        @pl.loop(0, BLOCKS)
        def _(block):
            total[block] = jnp.zeros((2, TILE, TILE), F32)

        for part in range(parts):

            @pl.loop(0, each)
            def _(slot):
                place = second_table[part * each + slot]

                @pl.when(place >= 0)
                def _():
                    total[place] += second_refs[part][slot].astype(F32)

        for part in range(CHUNKS):
            copies[part].wait()

            @pl.loop(part * chunk, (part + 1) * chunk)
            def _(slot):
                place = main_table[slot]

                @pl.when(place >= 0)
                def _():
                    total[place] += held[slot].astype(F32)

        @pl.loop(0, BLOCKS)
        def _(block):
            rows = pl.ds(pl.multiple_of((block // SIDE) * TILE, TILE), TILE)
            cols = pl.ds(pl.multiple_of((block % SIDE) * TILE, TILE), TILE)
            gen_ref[rows, cols] = total[block, 0].astype(BF16)
            ham_ref[rows, cols] = total[block, 1].astype(BF16)

    outs = [jax.ShapeDtypeStruct((SIDE * TILE, SIDE * TILE), BF16)] * 2
    scratch = [
        pltpu.VMEM((BLOCKS, 2, TILE, TILE), F32),
        pltpu.VMEM(main.shape, BF16),
        pltpu.SemaphoreType.DMA((CHUNKS,)),
    ]
    tables, arrays = (main_offsets, second_offsets), (main, *seconds)
    return kernel_call(body, tables, arrays, outs, scratch, far_in=1)


def back_tiles(main_offsets, second_offsets, pieces, cross):
    count = len(RELATIVE)

    chunk = CHAN // CHUNKS

    def body(main_table, second_table, piece_table, cross_ref, upper_ref, lower_ref, *refs):
        piece_refs, (held, done) = refs[:count], refs[count:]
        copies = []
        for part in range(CHUNKS):

            @pl.loop(part * chunk, (part + 1) * chunk)
            def _(slot):
                tile = tile_at(cross_ref, main_table[slot]).astype(BF16)
                held[slot] = tile[:UPPER]
                lower_ref[slot] = tile[UPPER:]

            where = pl.ds(part * chunk, chunk)
            copies.append(pltpu.make_async_copy(held.at[where], upper_ref.at[where], done.at[part]))
            copies[-1].start()

        @pl.loop(0, CHAN, unroll=4)
        def _(slot):
            block = second_table[slot]
            row = (block // SIDE) * TILE
            col = pl.multiple_of((block % SIDE) * TILE, TILE)
            for part in range(count):
                first = pl.multiple_of(row + piece_table[part] * PIECE, PIECE)
                rows = cross_ref[pl.ds(first, PIECE), pl.ds(col, TILE)]
                piece_refs[part][slot] = rows.astype(BF16)

        for copy in copies:
            copy.wait()

    outs = [
        pltpu.HBM((CHAN, UPPER, TILE), BF16),
        jax.ShapeDtypeStruct((CHAN, TILE - UPPER, TILE), BF16),
    ]
    scratch = [pltpu.VMEM(outs[0].shape, BF16), pltpu.SemaphoreType.DMA((CHUNKS,))]
    outs += [jax.ShapeDtypeStruct((CHAN, PIECE, TILE), BF16)] * count
    tables = (main_offsets, second_offsets, pieces)
    return kernel_call(body, tables, (cross,), outs, scratch, far_out=1)


def back_direct(main_offsets, second_offsets, cross):
    def body(main_table, second_table, cross_ref, out_ref):
        @pl.loop(0, CHAN)
        def _(slot):
            out_ref[slot, 0] = tile_at(cross_ref, main_table[slot]).astype(BF16)
            out_ref[slot, 1] = tile_at(cross_ref, second_table[slot]).astype(BF16)

    out = jax.ShapeDtypeStruct((CHAN, 2, TILE, TILE), BF16)
    return kernel_call(body, (main_offsets, second_offsets), (cross,), out)


def joined(choice, lower, routed):
    rows, parts = TILE - UPPER, len(routed)

    def body(table, lower_ref, *refs):
        routed_refs, (out_ref, held) = refs[:parts], refs[parts:]

        @pl.loop(0, CHAN)
        def _(slot):
            for part in range(parts):
                held[part, slot] = routed_refs[part][slot]

        @pl.loop(0, CHAN)
        def _(slot):
            out_ref[slot, :rows] = lower_ref[slot]
            out_ref[slot, rows:] = held[table[slot], slot]

    out = pltpu.HBM((CHAN, rows + PIECE, TILE), BF16)
    scratch = [pltpu.VMEM((parts, CHAN, PIECE, TILE), BF16)]
    return kernel_call(body, (choice,), (lower, *routed), out, scratch)


def gathered(slots, main):
    def body(table, main_ref, out_ref):
        @pl.loop(0, BLOCKS)
        def _(block):
            slot = table[block]

            @pl.when(slot >= 0)
            def _():
                out_ref[block] = main_ref[slot]

    out = jax.ShapeDtypeStruct((BLOCKS, *main.shape[1:]), BF16)
    return kernel_call(body, (slots,), (main,), out)


def in_bands(tiles):
    rows = TILE - UPPER

    def body(tile_ref, upper_ref, lower_ref):
        @pl.loop(0, BLOCKS)
        def _(block):
            tile = tile_ref[block]
            upper_ref[block] = tile[:UPPER]
            lower_ref[block] = tile[UPPER:]

    outs = [
        jax.ShapeDtypeStruct((BLOCKS, UPPER, TILE), BF16),
        jax.ShapeDtypeStruct((BLOCKS + Z * (UPPER // rows), rows, TILE), BF16),
    ]
    return kernel_call(body, (), (tiles,), outs)


def gathered_lower(slots, planes, main):
    rows = TILE - UPPER
    units, pieces = UPPER // rows, rows // PIECE

    def body(table, plane_table, main_ref, out_ref):
        @pl.loop(0, BLOCKS)
        def _(block):
            slot, plane = table[block], plane_table[block]

            @pl.when(slot >= 0)
            def _():
                out_ref[block] = main_ref[slot, :rows]

            @pl.when(slot < 0)
            def _():
                for part in range(pieces):
                    where = part + UPPER // PIECE
                    source = chan_of(where // CORE, plane, where % CORE)
                    out_ref[block, pl.ds(part * PIECE, PIECE)] = main_ref[source, rows:]

        @pl.loop(0, Z)
        def _(plane):
            for unit in range(units):
                for part in range(pieces):
                    where = unit * pieces + part
                    source = chan_of(where // CORE, plane, where % CORE)
                    unit_rows = pl.ds(part * PIECE, PIECE)
                    out_ref[BLOCKS + plane * units + unit, unit_rows] = main_ref[source, rows:]

    out = jax.ShapeDtypeStruct((BLOCKS + Z * units, rows, TILE), BF16)
    return kernel_call(body, (slots, planes), (main,), out)


def whole_tile(block, plane, upper, upper_block, lower):
    units = UPPER // (TILE - UPPER)
    late = lower[pl.ds(BLOCKS + jnp.maximum(plane, 0) * units, units)].reshape(UPPER, TILE)
    top = jnp.where(plane >= 0, late, upper[upper_block])
    return jnp.concatenate([top, lower[block]])


def by_bands(body, table, full, upper, upper_spec, lower, kind):
    side = SIDE * TILE
    band = pl.BlockSpec((TILE, side), lambda i: (i, 0))
    return pl.pallas_call(
        body,
        grid=(SIDE,),
        out_shape=kind((side, side), F32),
        in_specs=[SMEM, band, upper_spec, pl.BlockSpec(lower.shape, lambda i: (0, 0, 0))],
        out_specs=band,
        compiler_params=pltpu.CompilerParams(vmem_limit_bytes=12 << 20),
    )(table, full, upper, lower)


def plus_own(planes, ladder, upper, lower):
    def body(table, ladder_ref, upper_ref, lower_ref, out_ref):
        i = pl.program_id(0)

        @pl.loop(0, SIDE)
        def _(j):
            cols = pl.ds(pl.multiple_of(j * TILE, TILE), TILE)
            block = i * SIDE + j
            tile = whole_tile(block, table[block], upper_ref, j, lower_ref)
            out_ref[:, cols] = ladder_ref[:, cols] + tile.astype(F32)

    upper_spec = pl.BlockSpec((SIDE, UPPER, TILE), lambda i: (i, 0, 0))
    return by_bands(body, planes, ladder, upper, upper_spec, lower, jax.ShapeDtypeStruct)


def minus_mirror(planes, base, upper, lower):
    def body(table, base_ref, upper_ref, lower_ref, out_ref):
        i = pl.program_id(0)

        @pl.loop(0, SIDE)
        def _(j):
            cols = pl.ds(pl.multiple_of(j * TILE, TILE), TILE)
            block = j * SIDE + i
            tile = whole_tile(block, table[block], upper_ref, block, lower_ref)
            out_ref[:, cols] = base_ref[:, cols] - tile.T.astype(F32)

    upper_spec = pl.BlockSpec(upper.shape, lambda i: (0, 0, 0))
    return by_bands(body, planes, base, upper, upper_spec, lower, pltpu.HBM)


def pair_product(left_a, right_a, left_b, right_b):
    first = jnp.dot(left_a, right_a, preferred_element_type=F32)
    return first - jnp.dot(left_b, right_b, preferred_element_type=F32)


def commutator_by_rows(gen, ham):
    def body(gen_rows, ham_rows, gen_ref, ham_ref, out_ref):
        first = jnp.dot(gen_rows[...], ham_ref[...], preferred_element_type=F32)
        out_ref[...] = first - jnp.dot(ham_rows[...], gen_ref[...], preferred_element_type=F32)

    band = pl.BlockSpec((TILE, SIDE * TILE), lambda i: (i, 0))
    whole = pl.BlockSpec(gen.shape, lambda i: (0, 0))
    return pl.pallas_call(
        body,
        grid=(SIDE,),
        out_shape=jax.ShapeDtypeStruct(gen.shape, F32),
        in_specs=[band, band, whole, whole],
        out_specs=band,
        compiler_params=pltpu.CompilerParams(vmem_limit_bytes=LIMIT << 20),
    )(gen, ham, gen, ham)


def ladder_term(gen_mat, ham_mat, occ_row):
    gen_occ = (gen_mat.astype(F32) * occ_row[None, :]).astype(BF16)
    ham_occ = (ham_mat.astype(F32) * occ_row[None, :]).astype(BF16)
    return pair_product(gen_occ, ham_mat, ham_occ, gen_mat)


def homes_of(owner_map):
    names = jnp.arange(CHAN, dtype=jnp.int32)
    tiles = jnp.sum((owner_map[..., None] == names).astype(jnp.int32), axis=-2)
    double = tiles == 2
    load = jnp.sum(double.astype(jnp.int32), axis=-2)
    mine, other = load[..., :, None], load[..., None, :]
    ahead = (other > mine) | ((other == mine) & (names[None, :] < names[:, None]))
    rank = jnp.sum(ahead.astype(jnp.int32), axis=-1)
    return rank, double


def on_device(generator, hamiltonian, occupation, owner, offset):
    gen_mat, ham_mat, occ_row = generator[0, 0], hamiltonian[0, 0], occupation[0, 0]
    me, grp = lax.axis_index("chan"), lax.axis_index("grp")
    my_x, my_z, my_core = me // (Z * CORE), (me // CORE) % Z, me % CORE
    owner_all = owner[:, :, :, 0]
    owners = lax.dynamic_index_in_dim(owner_all, grp, 0, keepdims=False)
    offsets = lax.dynamic_index_in_dim(offset, grp, 0, keepdims=False)
    names = jnp.arange(CHAN, dtype=jnp.int32)
    blocks = jnp.arange(BLOCKS, dtype=jnp.int32)
    steps = jnp.arange(Z, dtype=jnp.int32)

    def home_of(rank):
        row, col = rank // Z, rank % Z
        return chan_of(row // CORE, col, row % CORE)

    home = home_of(homes_of(owners)[0])

    def routes(named):
        dest = jnp.sum(jnp.where(named[..., None] == names, home, 0), axis=-1)
        alike = named[..., None, :] == named[..., :, None]
        return dest, jnp.any(alike & (blocks[None, :] < blocks[:, None]), axis=-1)

    my_dest, my_later = routes(lax.dynamic_index_in_dim(owners, me, 0, keepdims=False))
    my_plane = (my_dest // CORE) % Z
    to_home = my_dest[None, :] == names[:, None]
    main_blocks = jnp.max(jnp.where(to_home & ~my_later, blocks, 0), axis=1)
    direct_blocks = jnp.max(jnp.where(to_home & my_later, blocks, 0), axis=1)
    hops = jnp.array(HOPS, jnp.int32)
    to_plane = my_plane[None, :] == ((my_z + hops) % Z)[:, None]
    second_blocks = jnp.max(jnp.where(to_plane & my_later, blocks, 0), axis=1)

    main_send, *second_send = send_tiles(main_blocks, second_blocks, gen_mat, ham_mat)
    second_send[0], owner_late, owners_late = lax.optimization_barrier(
        (second_send[0], owner_all, owners)
    )
    dest, later = routes(owners_late)
    rank_all, double_all = homes_of(owner_late)
    planes_all = ((rank_all % Z)[..., None] == steps).astype(BF16)
    in_plane = jnp.einsum("gck,gkt->gct", double_all.astype(BF16), planes_all, preferred_element_type=F32)
    crowded = jnp.max(in_plane) > 1.5

    shifted = [z_shift(second_send[i], HOPS[i]) for i in range(1, Z)]
    main = exchanged(main_send)
    ladder = ladder_term(gen_mat, ham_mat, occ_row)

    second_z = jnp.stack([second_send[0]] + shifted)
    same = [second_z] + [x_shift(second_z, s, 0) for s in range(1, X)]
    seconds = same + [x_shift(part, 0, 1) for part in same]

    here = dest == me
    main_place = jnp.max(jnp.where(here & ~later, offsets, -1), axis=1)
    second_place = jnp.max(jnp.where(here & later, offsets, -1), axis=1)
    flips = jnp.arange(CORE, dtype=jnp.int32)[:, None]
    shifts = jnp.arange(X, dtype=jnp.int32)[None, :]
    from_z = (my_z - hops) % Z
    came_from = chan_of(((my_x - shifts) % X)[..., None], from_z, (my_core ^ flips)[..., None]).reshape(-1)
    place_in = jnp.sum(jnp.where(came_from[:, None] == names, second_place, 0), axis=1)

    mirror = [(g, g ^ 1) for g in range(lax.axis_size("grp"))]
    slots = jnp.where(my_later, -1, my_dest)
    own_planes = jnp.where(my_later, my_plane, -1)

    def of_partner(array):
        return lax.dynamic_index_in_dim(array, grp ^ 1, 0, keepdims=False)

    named = lax.dynamic_index_in_dim(of_partner(owner_late), me, 0, keepdims=False)
    named_one = (named[:, None] == names).astype(BF16)
    named_plane = jnp.dot(named_one, of_partner(planes_all), preferred_element_type=F32)
    named_plane = jnp.sum(named_plane.astype(jnp.int32) * steps, axis=-1)
    named_later = jnp.any((named[None, :] == named[:, None]) & (blocks[None, :] < blocks[:, None]), axis=-1)
    partner_planes = jnp.where(named_later, named_plane, -1)

    main, ladder, crowded, slots, own_planes, partner_planes = lax.optimization_barrier(
        (main, ladder, crowded, slots, own_planes, partner_planes)
    )
    gen_full, ham_full = placed(main_place, place_in, main, seconds)
    cross = pair_product(gen_full, ham_full, ham_full, gen_full)
    back_main_offsets = jnp.maximum(main_place, 0)

    piece_of = (((my_x + shifts) % X) * CORE + (my_core ^ flips)).reshape(-1)
    upper_send, lower_rows, *pieces = back_tiles(
        back_main_offsets, jnp.maximum(second_place, 0), piece_of, cross
    )
    upper = exchanged(upper_send)
    routed = [
        x_shift(piece, step, flip) if step or flip else piece
        for (step, flip), piece in zip(RELATIVE, pieces)
    ]
    in_my_plane = later & ((dest // CORE) % Z == my_z)
    holder = jnp.max(jnp.where(in_my_plane, dest, 0), axis=1)
    choice = ((holder % CORE) ^ my_core) * X + (my_x - holder // (Z * CORE)) % X
    lower_send = joined(choice, lower_rows, routed)
    lower = exchanged(lower_send)

    upper_own = gathered(slots, upper)
    upper_partner = lax.ppermute(upper_own, "grp", mirror)
    lower_own = gathered_lower(slots, jnp.maximum(own_planes, 0), lower)
    lower_partner = lax.ppermute(lower_own, "grp", mirror)

    base = plus_own(own_planes, ladder, upper_own, lower_own)

    def fast():
        return minus_mirror(partner_planes, base, upper_partner, lower_partner)

    def slow():
        arrived = exchanged(direct_tiles(direct_blocks, gen_mat, ham_mat))
        gen_slow, ham_slow = placed(main_place, second_place, main, [arrived])
        cross_slow = commutator_by_rows(gen_slow, ham_slow)
        back = exchanged(back_direct(back_main_offsets, jnp.maximum(second_place, 0), cross_slow))
        back = back.reshape(2 * CHAN, TILE, TILE)
        own = gathered(2 * my_dest + my_later.astype(jnp.int32), back)
        partner = in_bands(lax.ppermute(own, "grp", mirror))
        nowhere = jnp.full((BLOCKS,), -1, jnp.int32)
        return minus_mirror(nowhere, plus_own(nowhere, ladder, *in_bands(own)), *partner)

    return lax.cond(crowded, slow, fast)[None, None]


def solution(mesh):
    in_specs = (
        P("grp", "chan", None, None),
        P("grp", "chan", None, None),
        P("grp", "chan", None),
        P(),
        P(),
    )
    out_specs = P("grp", "chan", None, None)

    return jax.shard_map(
        on_device, mesh=mesh, in_specs=in_specs, out_specs=out_specs, check_vma=False
    )
```

```python
import jax
import jax.numpy as jnp
from jax import lax
from jax.experimental import pallas as pl
from jax.experimental.pallas import tpu as pltpu
from jax.sharding import PartitionSpec as P


TILE = 128
SIDE = 7
BLOCKS = SIDE * SIDE
X, Z, CORE = 4, 8, 2
CHAN = X * Z * CORE
UPPER = 112
LIMIT = 24
PIECE = TILE // (X * CORE)
HOPS = tuple(range(Z))
RELATIVE = [(step, flip) for flip in range(CORE) for step in range(X)]
F32, BF16 = jnp.float32, jnp.bfloat16


SMEM = pl.BlockSpec(memory_space=pltpu.SMEM)
VMEM = pl.BlockSpec(memory_space=pltpu.VMEM)
HBM = pl.BlockSpec(memory_space=pltpu.HBM)
CHUNKS = 4


def chan_of(x, z, core):
    return (x * Z + z) * CORE + core


def z_shift(value, step):
    pairs = [
        (chan_of(x, z, c), chan_of(x, (z + step) % Z, c))
        for x in range(X)
        for z in range(Z)
        for c in range(CORE)
    ]
    return lax.ppermute(value, "chan", pairs)


def x_shift(value, step, flip):
    pairs = [
        (chan_of(x, z, c), chan_of((x + step) % X, z, c ^ flip))
        for x in range(X)
        for z in range(Z)
        for c in range(CORE)
    ]
    return lax.ppermute(value, "chan", pairs)


def exchanged(value):
    return lax.all_to_all(value, "chan", split_axis=0, concat_axis=0, tiled=True)


def kernel_call(body, tables, arrays, outs, scratch=(), far_in=0, far_out=0, limit=12):
    out_specs = VMEM
    if isinstance(outs, list):
        out_specs = [HBM] * far_out + [VMEM] * (len(outs) - far_out)
    return pl.pallas_call(
        body,
        out_shape=outs,
        in_specs=[SMEM] * len(tables) + [HBM] * far_in + [VMEM] * (len(arrays) - far_in),
        out_specs=out_specs,
        scratch_shapes=list(scratch),
        compiler_params=pltpu.CompilerParams(vmem_limit_bytes=limit << 20),
    )(*tables, *arrays)


def tile_at(ref, block):
    row = pl.multiple_of((block // SIDE) * TILE, TILE)
    col = pl.multiple_of((block % SIDE) * TILE, TILE)
    return ref[pl.ds(row, TILE), pl.ds(col, TILE)]


def send_tiles(main_blocks, second_blocks, gen, ham):
    count = second_blocks.shape[0]
    chunk = CHAN // CHUNKS

    def body(main_table, second_table, gen_ref, ham_ref, main_ref, *refs):
        second_refs, (held, done) = refs[:count], refs[count:]
        copies = []
        for part in range(CHUNKS):

            @pl.loop(part * chunk, (part + 1) * chunk)
            def _(slot):
                block = main_table[slot]
                held[slot, 0] = tile_at(gen_ref, block)
                held[slot, 1] = tile_at(ham_ref, block)

            where = pl.ds(part * chunk, chunk)
            copies.append(pltpu.make_async_copy(held.at[where], main_ref.at[where], done.at[part]))
            copies[-1].start()
        for step in range(count):
            block = second_table[step]
            second_refs[step][0] = tile_at(gen_ref, block)
            second_refs[step][1] = tile_at(ham_ref, block)
        for copy in copies:
            copy.wait()

    outs = [pltpu.HBM((CHAN, 2, TILE, TILE), BF16)]
    scratch = [pltpu.VMEM(outs[0].shape, BF16), pltpu.SemaphoreType.DMA((CHUNKS,))]
    outs += [jax.ShapeDtypeStruct((2, TILE, TILE), BF16)] * count
    return kernel_call(body, (main_blocks, second_blocks), (gen, ham), outs, scratch, far_out=1)


def direct_tiles(blocks, gen, ham):
    def body(table, gen_ref, ham_ref, out_ref):
        @pl.loop(0, CHAN)
        def _(slot):
            block = table[slot]
            out_ref[slot, 0] = tile_at(gen_ref, block)
            out_ref[slot, 1] = tile_at(ham_ref, block)

    out = jax.ShapeDtypeStruct((CHAN, 2, TILE, TILE), BF16)
    return kernel_call(body, (blocks,), (gen, ham), out)


def placed(main_offsets, second_offsets, main, seconds):
    parts = len(seconds)
    each = seconds[0].shape[0]
    chunk = CHAN // CHUNKS

    def body(main_table, second_table, main_ref, *refs):
        second_refs, (gen_ref, ham_ref, total, held, done) = refs[:parts], refs[parts:]
        copies = []
        for part in range(CHUNKS):
            where = pl.ds(part * chunk, chunk)
            copies.append(pltpu.make_async_copy(main_ref.at[where], held.at[where], done.at[part]))
            copies[-1].start()

        @pl.loop(0, BLOCKS)
        def _(block):
            total[block] = jnp.zeros((2, TILE, TILE), F32)

        for part in range(parts):

            @pl.loop(0, each)
            def _(slot):
                place = second_table[part * each + slot]

                @pl.when(place >= 0)
                def _():
                    total[place] += second_refs[part][slot].astype(F32)

        for part in range(CHUNKS):
            copies[part].wait()

            @pl.loop(part * chunk, (part + 1) * chunk)
            def _(slot):
                place = main_table[slot]

                @pl.when(place >= 0)
                def _():
                    total[place] += held[slot].astype(F32)

        @pl.loop(0, SIDE)
        def _(i):
            rows = pl.ds(pl.multiple_of(i * TILE, TILE), TILE)
            for j in range(SIDE):
                cols = pl.ds(j * TILE, TILE)
                gen_ref[rows, cols] = total[i * SIDE + j, 0].astype(BF16)
                ham_ref[rows, cols] = total[i * SIDE + j, 1].astype(BF16)

    outs = [jax.ShapeDtypeStruct((SIDE * TILE, SIDE * TILE), BF16)] * 2
    scratch = [
        pltpu.VMEM((BLOCKS, 2, TILE, TILE), F32),
        pltpu.VMEM(main.shape, BF16),
        pltpu.SemaphoreType.DMA((CHUNKS,)),
    ]
    tables, arrays = (main_offsets, second_offsets), (main, *seconds)
    return kernel_call(body, tables, arrays, outs, scratch, far_in=1, limit=24)


def back_tiles(main_offsets, second_offsets, pieces, cross):
    count = len(RELATIVE)

    chunk = CHAN // CHUNKS

    def body(main_table, second_table, piece_table, cross_ref, upper_ref, lower_ref, *refs):
        piece_refs, (held, done) = refs[:count], refs[count:]
        copies = []
        for part in range(CHUNKS):

            @pl.loop(part * chunk, (part + 1) * chunk)
            def _(slot):
                tile = tile_at(cross_ref, main_table[slot]).astype(BF16)
                held[slot] = tile[:UPPER]
                lower_ref[slot] = tile[UPPER:]

            where = pl.ds(part * chunk, chunk)
            copies.append(pltpu.make_async_copy(held.at[where], upper_ref.at[where], done.at[part]))
            copies[-1].start()

        @pl.loop(0, CHAN, unroll=2)
        def _(slot):
            block = second_table[slot]
            row = (block // SIDE) * TILE
            col = pl.multiple_of((block % SIDE) * TILE, TILE)
            for part in range(count):
                first = pl.multiple_of(row + piece_table[part] * PIECE, PIECE)
                rows = cross_ref[pl.ds(first, PIECE), pl.ds(col, TILE)]
                piece_refs[part][slot] = rows.astype(BF16)

        for copy in copies:
            copy.wait()

    outs = [
        pltpu.HBM((CHAN, UPPER, TILE), BF16),
        jax.ShapeDtypeStruct((CHAN, TILE - UPPER, TILE), BF16),
    ]
    scratch = [pltpu.VMEM(outs[0].shape, BF16), pltpu.SemaphoreType.DMA((CHUNKS,))]
    outs += [jax.ShapeDtypeStruct((CHAN, PIECE, TILE), BF16)]
    outs += [pltpu.HBM((CHAN, PIECE, TILE), BF16)] * (count - 1)
    tables = (main_offsets, second_offsets, pieces)
    return kernel_call(body, tables, (cross,), outs, scratch, far_out=1)


def back_direct(main_offsets, second_offsets, cross):
    def body(main_table, second_table, cross_ref, out_ref):
        @pl.loop(0, CHAN)
        def _(slot):
            out_ref[slot, 0] = tile_at(cross_ref, main_table[slot]).astype(BF16)
            out_ref[slot, 1] = tile_at(cross_ref, second_table[slot]).astype(BF16)

    out = jax.ShapeDtypeStruct((CHAN, 2, TILE, TILE), BF16)
    return kernel_call(body, (main_offsets, second_offsets), (cross,), out)


def joined(choice, lower, routed):
    rows, parts = TILE - UPPER, len(routed)

    def body(table, lower_ref, *refs):
        routed_refs, (out_ref, held) = refs[:parts], refs[parts:]

        @pl.loop(0, CHAN)
        def _(slot):
            for part in range(parts):
                held[part, slot] = routed_refs[part][slot]

        @pl.loop(0, CHAN)
        def _(slot):
            out_ref[slot, :rows] = lower_ref[slot]
            out_ref[slot, rows:] = held[table[slot], slot]

    out = pltpu.HBM((CHAN, rows + PIECE, TILE), BF16)
    scratch = [pltpu.VMEM((parts, CHAN, PIECE, TILE), BF16)]
    return kernel_call(body, (choice,), (lower, *routed), out, scratch)


def gathered(slots, main):
    def body(table, main_ref, out_ref):
        @pl.loop(0, BLOCKS)
        def _(block):
            slot = table[block]

            @pl.when(slot >= 0)
            def _():
                out_ref[block] = main_ref[slot]

    out = jax.ShapeDtypeStruct((BLOCKS, *main.shape[1:]), BF16)
    return kernel_call(body, (slots,), (main,), out)


def in_bands(tiles):
    rows = TILE - UPPER

    def body(tile_ref, upper_ref, lower_ref):
        @pl.loop(0, BLOCKS)
        def _(block):
            tile = tile_ref[block]
            upper_ref[block] = tile[:UPPER]
            lower_ref[block] = tile[UPPER:]

    outs = [
        jax.ShapeDtypeStruct((BLOCKS, UPPER, TILE), BF16),
        jax.ShapeDtypeStruct((BLOCKS + Z * (UPPER // rows), rows, TILE), BF16),
    ]
    return kernel_call(body, (), (tiles,), outs)


def gathered_lower(slots, planes, main):
    rows = TILE - UPPER
    units, pieces = UPPER // rows, rows // PIECE

    def body(table, plane_table, main_ref, out_ref):
        @pl.loop(0, BLOCKS)
        def _(block):
            slot, plane = table[block], plane_table[block]

            @pl.when(slot >= 0)
            def _():
                out_ref[block] = main_ref[slot, :rows]

            @pl.when(slot < 0)
            def _():
                for part in range(pieces):
                    where = part + UPPER // PIECE
                    source = chan_of(where // CORE, plane, where % CORE)
                    out_ref[block, pl.ds(part * PIECE, PIECE)] = main_ref[source, rows:]

        @pl.loop(0, Z)
        def _(plane):
            for unit in range(units):
                for part in range(pieces):
                    where = unit * pieces + part
                    source = chan_of(where // CORE, plane, where % CORE)
                    unit_rows = pl.ds(part * PIECE, PIECE)
                    out_ref[BLOCKS + plane * units + unit, unit_rows] = main_ref[source, rows:]

    out = jax.ShapeDtypeStruct((BLOCKS + Z * units, rows, TILE), BF16)
    return kernel_call(body, (slots, planes), (main,), out)


def whole_tile(block, plane, upper, upper_block, lower):
    units = UPPER // (TILE - UPPER)
    late = lower[pl.ds(BLOCKS + jnp.maximum(plane, 0) * units, units)].reshape(UPPER, TILE)
    top = jnp.where(plane >= 0, late, upper[upper_block])
    return jnp.concatenate([top, lower[block]])


def by_bands(body, table, full, upper, upper_spec, lower, kind):
    side = SIDE * TILE
    band = pl.BlockSpec((TILE, side), lambda i: (i, 0))
    return pl.pallas_call(
        body,
        grid=(SIDE,),
        out_shape=kind((side, side), F32),
        in_specs=[SMEM, band, upper_spec, pl.BlockSpec(lower.shape, lambda i: (0, 0, 0))],
        out_specs=band,
        compiler_params=pltpu.CompilerParams(vmem_limit_bytes=12 << 20),
    )(table, full, upper, lower)


def plus_own(planes, ladder, upper, lower):
    def body(table, ladder_ref, upper_ref, lower_ref, out_ref):
        i = pl.program_id(0)

        @pl.loop(0, SIDE)
        def _(j):
            cols = pl.ds(pl.multiple_of(j * TILE, TILE), TILE)
            block = i * SIDE + j
            tile = whole_tile(block, table[block], upper_ref, j, lower_ref)
            out_ref[:, cols] = ladder_ref[:, cols] + tile.astype(F32)

    upper_spec = pl.BlockSpec((SIDE, UPPER, TILE), lambda i: (i, 0, 0))
    return by_bands(body, planes, ladder, upper, upper_spec, lower, jax.ShapeDtypeStruct)


def minus_mirror(planes, base, upper, lower, unroll=1):
    def body(table, base_ref, upper_ref, lower_ref, out_ref):
        i = pl.program_id(0)

        @pl.loop(0, SIDE)
        def _(j):
            cols = pl.ds(pl.multiple_of(j * TILE, TILE), TILE)
            block = j * SIDE + i
            tile = whole_tile(block, table[block], upper_ref, block, lower_ref)
            out_ref[:, cols] = base_ref[:, cols] - tile.T.astype(F32)

    upper_spec = pl.BlockSpec(upper.shape, lambda i: (0, 0, 0))
    return by_bands(body, planes, base, upper, upper_spec, lower, pltpu.HBM)


def pair_product(left_a, right_a, left_b, right_b):
    first = jnp.dot(left_a, right_a, preferred_element_type=F32)
    return first - jnp.dot(left_b, right_b, preferred_element_type=F32)


def commutator_by_rows(gen, ham):
    def body(gen_rows, ham_rows, gen_ref, ham_ref, out_ref):
        first = jnp.dot(gen_rows[...], ham_ref[...], preferred_element_type=F32)
        out_ref[...] = first - jnp.dot(ham_rows[...], gen_ref[...], preferred_element_type=F32)

    band = pl.BlockSpec((TILE, SIDE * TILE), lambda i: (i, 0))
    whole = pl.BlockSpec(gen.shape, lambda i: (0, 0))
    return pl.pallas_call(
        body,
        grid=(SIDE,),
        out_shape=jax.ShapeDtypeStruct(gen.shape, F32),
        in_specs=[band, band, whole, whole],
        out_specs=band,
        compiler_params=pltpu.CompilerParams(vmem_limit_bytes=LIMIT << 20),
    )(gen, ham, gen, ham)


def ladder_term(gen_mat, ham_mat, occ_row):
    gen_occ = (gen_mat.astype(F32) * occ_row[None, :]).astype(BF16)
    ham_occ = (ham_mat.astype(F32) * occ_row[None, :]).astype(BF16)
    return pair_product(gen_occ, ham_mat, ham_occ, gen_mat)


def homes_of(owner_map):
    names = jnp.arange(CHAN, dtype=jnp.int32)
    tiles = jnp.sum((owner_map[..., None] == names).astype(jnp.int32), axis=-2)
    double = tiles == 2
    load = jnp.sum(double.astype(jnp.int32), axis=-2)
    mine, other = load[..., :, None], load[..., None, :]
    ahead = (other > mine) | ((other == mine) & (names[None, :] < names[:, None]))
    rank = jnp.sum(ahead.astype(jnp.int32), axis=-1)
    return rank, double


def on_device(generator, hamiltonian, occupation, owner, offset):
    gen_mat, ham_mat, occ_row = generator[0, 0], hamiltonian[0, 0], occupation[0, 0]
    me, grp = lax.axis_index("chan"), lax.axis_index("grp")
    my_x, my_z, my_core = me // (Z * CORE), (me // CORE) % Z, me % CORE
    owner_all = owner[:, :, :, 0]
    owners = lax.dynamic_index_in_dim(owner_all, grp, 0, keepdims=False)
    offsets = lax.dynamic_index_in_dim(offset, grp, 0, keepdims=False)
    names = jnp.arange(CHAN, dtype=jnp.int32)
    blocks = jnp.arange(BLOCKS, dtype=jnp.int32)
    steps = jnp.arange(Z, dtype=jnp.int32)

    def home_of(rank):
        row, col = rank // Z, rank % Z
        return chan_of(row // CORE, col, row % CORE)

    home = home_of(homes_of(owners)[0])

    def routes(named):
        dest = jnp.sum(jnp.where(named[..., None] == names, home, 0), axis=-1)
        alike = named[..., None, :] == named[..., :, None]
        return dest, jnp.any(alike & (blocks[None, :] < blocks[:, None]), axis=-1)

    my_dest, my_later = routes(lax.dynamic_index_in_dim(owners, me, 0, keepdims=False))
    my_plane = (my_dest // CORE) % Z
    to_home = my_dest[None, :] == names[:, None]
    main_blocks = jnp.max(jnp.where(to_home & ~my_later, blocks, 0), axis=1)
    direct_blocks = jnp.max(jnp.where(to_home & my_later, blocks, 0), axis=1)
    hops = jnp.array(HOPS, jnp.int32)
    to_plane = my_plane[None, :] == ((my_z + hops) % Z)[:, None]
    second_blocks = jnp.max(jnp.where(to_plane & my_later, blocks, 0), axis=1)

    main_send, *second_send = send_tiles(main_blocks, second_blocks, gen_mat, ham_mat)
    second_send[0], owner_late, owners_late = lax.optimization_barrier(
        (second_send[0], owner_all, owners)
    )
    dest, later = routes(owners_late)
    rank_all, double_all = homes_of(owner_late)
    planes_all = ((rank_all % Z)[..., None] == steps).astype(BF16)
    in_plane = jnp.einsum("gck,gkt->gct", double_all.astype(BF16), planes_all, preferred_element_type=F32)
    crowded = jnp.max(in_plane) > 1.5

    shifted = [z_shift(second_send[i], HOPS[i]) for i in range(1, Z)]
    main = exchanged(main_send)
    ladder = ladder_term(gen_mat, ham_mat, occ_row)

    second_z = jnp.stack([second_send[0]] + shifted)
    same = [second_z] + [x_shift(second_z, s, 0) for s in range(1, X)]
    seconds = same + [x_shift(part, 0, 1) for part in same]

    here = dest == me
    main_place = jnp.max(jnp.where(here & ~later, offsets, -1), axis=1)
    second_place = jnp.max(jnp.where(here & later, offsets, -1), axis=1)
    flips = jnp.arange(CORE, dtype=jnp.int32)[:, None]
    shifts = jnp.arange(X, dtype=jnp.int32)[None, :]
    from_z = (my_z - hops) % Z
    came_from = chan_of(((my_x - shifts) % X)[..., None], from_z, (my_core ^ flips)[..., None]).reshape(-1)
    place_in = jnp.sum(jnp.where(came_from[:, None] == names, second_place, 0), axis=1)

    mirror = [(g, g ^ 1) for g in range(lax.axis_size("grp"))]
    slots = jnp.where(my_later, -1, my_dest)
    own_planes = jnp.where(my_later, my_plane, -1)

    def of_partner(array):
        return lax.dynamic_index_in_dim(array, grp ^ 1, 0, keepdims=False)

    named = lax.dynamic_index_in_dim(of_partner(owner_late), me, 0, keepdims=False)
    named_one = (named[:, None] == names).astype(BF16)
    named_plane = jnp.dot(named_one, of_partner(planes_all), preferred_element_type=F32)
    named_plane = jnp.sum(named_plane.astype(jnp.int32) * steps, axis=-1)
    named_later = jnp.any((named[None, :] == named[:, None]) & (blocks[None, :] < blocks[:, None]), axis=-1)
    partner_planes = jnp.where(named_later, named_plane, -1)

    main, ladder, crowded, slots, own_planes, partner_planes = lax.optimization_barrier(
        (main, ladder, crowded, slots, own_planes, partner_planes)
    )
    gen_full, ham_full = placed(main_place, place_in, main, seconds)
    cross = pair_product(gen_full, ham_full, ham_full, gen_full)
    back_main_offsets = jnp.maximum(main_place, 0)

    piece_of = (((my_x + shifts) % X) * CORE + (my_core ^ flips)).reshape(-1)
    upper_send, lower_rows, *pieces = back_tiles(
        back_main_offsets, jnp.maximum(second_place, 0), piece_of, cross
    )
    upper = exchanged(upper_send)
    routed = [
        x_shift(piece, step, flip) if step or flip else piece
        for (step, flip), piece in zip(RELATIVE, pieces)
    ]
    in_my_plane = later & ((dest // CORE) % Z == my_z)
    holder = jnp.max(jnp.where(in_my_plane, dest, 0), axis=1)
    choice = ((holder % CORE) ^ my_core) * X + (my_x - holder // (Z * CORE)) % X

    upper_own, lower_rows = lax.optimization_barrier((gathered(slots, upper), lower_rows))
    upper_partner = lax.ppermute(upper_own, "grp", mirror)
    lower_send = joined(choice, lower_rows, routed)
    lower = exchanged(lower_send)
    lower_own = gathered_lower(slots, jnp.maximum(own_planes, 0), lower)
    lower_partner = lax.ppermute(lower_own, "grp", mirror)

    base = plus_own(own_planes, ladder, upper_own, lower_own)

    def fast():
        return minus_mirror(partner_planes, base, upper_partner, lower_partner, unroll=SIDE)

    def slow():
        arrived = exchanged(direct_tiles(direct_blocks, gen_mat, ham_mat))
        gen_slow, ham_slow = placed(main_place, second_place, main, [arrived])
        cross_slow = commutator_by_rows(gen_slow, ham_slow)
        back = exchanged(back_direct(back_main_offsets, jnp.maximum(second_place, 0), cross_slow))
        back = back.reshape(2 * CHAN, TILE, TILE)
        own = gathered(2 * my_dest + my_later.astype(jnp.int32), back)
        partner = in_bands(lax.ppermute(own, "grp", mirror))
        nowhere = jnp.full((BLOCKS,), -1, jnp.int32)
        return minus_mirror(nowhere, plus_own(nowhere, ladder, *in_bands(own)), *partner)

    return lax.cond(crowded, slow, fast)[None, None]


def solution(mesh):
    in_specs = (
        P("grp", "chan", None, None),
        P("grp", "chan", None, None),
        P("grp", "chan", None),
        P(),
        P(),
    )
    out_specs = P("grp", "chan", None, None)

    return jax.shard_map(
        on_device, mesh=mesh, in_specs=in_specs, out_specs=out_specs, check_vma=False
    )
```
